128 devices in a mesh: grp: 4 (over z), dev: 32 (over y, x, core).
Axes of the slice: x: 4, y: 4, z: 4, core: 2. Of those that a mesh axis runs over, the one named last changes fastest.
Arguments:
- omega: float32 [4, 128, 256, 128], P('grp', 'dev'), may hold values from -6 to 6
- u_factor: float32 [4, 128, 80, 256, 32], P('grp', 'dev'), may hold values from -0.0625 to 0.0625
- v_factor: float32 [4, 128, 80, 256, 32], P('grp', 'dev'), may hold values from -0.375 to 0.375
- columns: int32 [4, 128, 80, 1], P('grp', 'dev'), may hold values from 0 to 127; in each aligned block of 320 rows (0 to 319, 320 to 639, ..., all dimensions but the last counted through in order) at most 3 rows name the same one
- ranks: int32 [4, 128, 80], P('grp', 'dev'), may hold values from 8 to 32
Outputs:
- leaf_basis: float32 [128, 256, 128], P('dev', 'grp')
- transfer: float32 [128, 256, 128], P('dev')
The draws below stay inside these ranges and needn't reach their ends.
Inputs may be any that keep to these rules, and one draw needn't show every extreme that they name: `columns`: within the 320 blocks of one device's row clusters in one group, at most 3 name any one column cluster, and some column cluster is named by exactly 3.
All inputs are finite; a program needn't handle non-finite values.
Results may differ from the reference program's by a relative error of at most 0.0003.
Values sent between devices are 32-bit elements; how exact they have to be, the bound alone decides.
A program may use at most 192 MiB of HBM per device.

```python
import math
import jax
import jax.numpy as jnp
import numpy as np
from jax import lax

CL = 4
NB = 80
LEAF = 256
K = 32
P_SIZE = 128
CLUSTERS = 128
MOSTC = 3
N_GRP = 4
N_DEV = 32


def plant(values, key, smallest, top_value):
    longest = values.shape.index(max(values.shape))
    spots = []
    for shift in (0, 1):
        where = [jax.random.randint(jax.random.fold_in(key, axis), (), 0, length) for axis, length in enumerate(values.shape)]
        where[longest] = (where[longest] + shift) % values.shape[longest]
        spots.append(tuple(where))
    return values.at[spots[0]].set(smallest).at[spots[1]].set(top_value)


def shard_levels(key, dims, cuts, smallest, top_value):
    def one(position, blocks):
        steps = jax.random.uniform(jax.random.fold_in(jax.random.fold_in(key, 6), position), (blocks,), jnp.float32, smallest / len(cuts), top_value / len(cuts))
        return jnp.repeat(jnp.exp(steps), dims[position] // blocks).reshape((-1,) + (1,) * (len(dims) - position - 1))

    gain = one(*cuts[0])
    for cut in cuts[1:]:
        gain = gain * one(*cut)
    return gain


def deal_out(stream_key, own, number, rows, count, top, most, slope):
    ranking = jax.random.permutation(stream_key, count)
    packed, ordinary = portions_of(count, rows * top, most, slope, True), portions_of(count, rows * top, most, slope, False)
    places = jnp.arange(count)

    def named(lengths, turn):
        used = int((lengths > 0).sum())
        fixed = max(1, used // 4)
        moved = fixed + (places - fixed + turn * (used - fixed)) % max(1, count - fixed)
        return jnp.zeros((count,), jnp.int32).at[ranking[jnp.where(places < fixed, places, moved)]].set(jnp.asarray(lengths, jnp.int32))

    lengths = jnp.where(number % 4 == 0, named(packed, number // 4), named(ordinary, number - number // 4 - 1))
    mixed = jax.random.permutation(jax.random.fold_in(own, 3), count)
    giver, receiver = mixed[0:count // 2 * 2:2], mixed[1:count // 2 * 2:2]
    slack = jnp.minimum(lengths[giver] - 1, most - lengths[receiver]) // 2
    slack = jnp.where((giver == ranking[0]) | (receiver == ranking[0]) | (lengths[receiver] == 0), 0, jnp.maximum(slack, 0))
    moved = jax.random.randint(jax.random.fold_in(own, 4), (count // 2,), 0, 1 << 20) % (slack + 1)
    lengths = lengths.at[giver].add(-moved).at[receiver].add(moved)
    items = jnp.searchsorted(jnp.cumsum(lengths), jnp.arange(rows * top), side="right").astype(jnp.int32)
    table = items.reshape(top, rows).T
    table = table[jax.random.permutation(jax.random.fold_in(own, 1), rows)]
    turn = jax.random.randint(jax.random.fold_in(own, 2), (rows, 1), 0, top)
    return jnp.take_along_axis(table, (jnp.arange(top)[None, :] + turn) % top, axis=1)


def portions_of(count, total, bound, lean, full):
    portions = [(1 << 20) // math.isqrt(grade ** lean) + 1 for grade in range(1, count + 1)]
    largest = bound if full else min(bound, max(-(-total // count), total * portions[0] // sum(portions)))
    least = 1 if total - largest >= count - 1 else 0
    counts, rest = [largest] + [least] * (count - 1), total - largest - least * (count - 1)
    while rest > 0:
        candidates = [i for i in range(1, count) if counts[i] < largest] or [i for i in range(1, count) if counts[i] < bound]
        pool, left = sum([portions[i] for i in candidates]), rest
        for i in candidates:
            addition = min(bound - counts[i], max(1, left * portions[i] // pool), rest)
            counts[i] = counts[i] + addition
            rest = rest - addition
    return np.array(counts)


def centred(own_key, shape, width, most, cuts=(), held_as=jnp.bfloat16):
    values = width * jax.random.normal(own_key, shape, jnp.float32)
    if cuts:
        values = values * shard_levels(own_key, shape, cuts, -0.22, 0.18)
    return jnp.clip(values, -most, most).astype(held_as)


def setup_inputs(seed: int = 0) -> dict:
    arg_keys = jax.random.split(jax.random.key(seed), 6)
    omega = centred(arg_keys[0], (N_GRP, CLUSTERS, LEAF, P_SIZE), 1.0, 6.0, ((0, 4), (1, 32)), jnp.float32)
    u_factor = centred(arg_keys[1], (N_GRP, CLUSTERS, NB, LEAF, K), (N_GRP * NB * K) ** -0.5, 0.0625, ((0, 4), (1, 32)), jnp.float32)
    v_factor = centred(arg_keys[2], (N_GRP, CLUSTERS, NB, LEAF, K), LEAF ** -0.5, 0.375, ((0, 4), (1, 32)), jnp.float32)
    columns_keys = jax.random.split(jax.random.fold_in(arg_keys[3], 1), N_GRP * CLUSTERS * NB // (CL * NB))
    columns_turns = jax.random.permutation(jax.random.fold_in(arg_keys[3], 3), N_GRP * CLUSTERS * NB // (CL * NB))
    columns = jax.vmap(lambda own, number: deal_out(jax.random.fold_in(arg_keys[3], 2), own, number, CL * NB, CLUSTERS, 1, MOSTC, 2))(columns_keys, columns_turns).reshape((N_GRP, CLUSTERS, NB, 1))
    ranks = plant(jax.random.randint(arg_keys[4], (N_GRP, CLUSTERS, NB), K // 4, K + 1), jax.random.fold_in(arg_keys[4], 1), K // 4, K).astype(jnp.int32)
    return {"omega": omega, "u_factor": u_factor, "v_factor": v_factor, "columns": columns, "ranks": ranks}


precise = lax.Precision.HIGHEST

def tree_node(left_factor, right_factor):
    gram_matrix = jnp.einsum('kp,kq->pq', left_factor, left_factor, precision=precise) + jnp.einsum('kp,kq->pq', right_factor, right_factor, precision=precise)
    lower_factor = jnp.linalg.cholesky(gram_matrix)
    stacked_rows = jnp.concatenate([left_factor, right_factor], axis=0)
    node_transfer = lax.linalg.triangular_solve(lower_factor, stacked_rows, left_side=False, lower=True, transpose_a=True)
    return (node_transfer, lower_factor.T)

def reference(omega, u_factor, v_factor, columns, ranks):
    sketch = jnp.zeros((CLUSTERS, LEAF, P_SIZE), jnp.float32)
    rank_index = jnp.arange(K, dtype=jnp.int32)
    for group_index in range(N_GRP):
        group_probe = omega[group_index]

        def cluster_sketch(pieces):
            u_rows, v_rows, col_ids, rank_vals = pieces
            rank_mask = (rank_index[None, :] < rank_vals[:, None]).astype(jnp.float32)
            coeff = jnp.einsum('bik,bip->bkp', v_rows, group_probe[col_ids], precision=precise)
            return jnp.einsum('bik,bkp->ip', u_rows * rank_mask[:, None, :], coeff, precision=precise)
        sketch = sketch + lax.map(cluster_sketch, (u_factor[group_index], v_factor[group_index], columns[group_index, :, :, 0], ranks[group_index]))
    gram_matrix = jnp.einsum('cip,ciq->cpq', sketch, sketch, precision=precise)
    lower_factor = jnp.linalg.cholesky(gram_matrix)
    leaf_basis = lax.linalg.triangular_solve(lower_factor, sketch, left_side=False, lower=True, transpose_a=True)
    factors = jnp.swapaxes(lower_factor, 1, 2)
    levels_out = []
    while factors.shape[0] > 1:
        made, factors = jax.vmap(tree_node)(factors[0::2], factors[1::2])
        levels_out.append(made)
    tree_part = jnp.zeros((N_DEV, 2 * P_SIZE, P_SIZE), jnp.float32)
    for depth_step, made in enumerate(levels_out[2:]):
        places = jnp.arange(made.shape[0], dtype=jnp.int32) * 2 ** (depth_step + 1) + (2 ** depth_step - 1)
        tree_part = tree_part.at[places].set(made)
    transfer = jnp.stack([levels_out[0][0::2], levels_out[0][1::2], levels_out[1], tree_part], axis=1)
    return (leaf_basis, transfer.reshape(CLUSTERS, 2 * P_SIZE, P_SIZE))
```

```python
import functools
import jax
import jax.numpy as jnp
from jax import lax
from jax.experimental import pallas as pl
from jax.experimental.pallas import tpu as pltpu
from jax.sharding import PartitionSpec as P

precise = lax.Precision.HIGHEST
fast = lax.Precision.HIGH


GROUP = 5
SEGS = ((0, 4), (4, 8), (8, 12), (12, 16))

def pick_lane(x, lane):
    idx = jnp.full(x.shape, lane, jnp.int32)
    return jnp.take_along_axis(x, idx, axis=1)

def factor_all(work, mats):
    sub = lax.broadcasted_iota(jnp.int32, (8, 128), 0)
    lane = lax.broadcasted_iota(jnp.int32, (8, 128), 1)

    def split(x):
        h = x.astype(jnp.bfloat16).astype(jnp.float32)
        rest = x - h
        d = rest.astype(jnp.bfloat16).astype(jnp.float32)
        return h, d, rest - d

    def panel(k, top):
        base = pl.multiple_of(k * 8, 8)
        raw = [work[m, pl.ds(base, 8), :] for m in mats]
        keep = lane >= base + sub
        below = lane >= base + 8
        prods = []
        rows = []
        for g in range(0, len(mats), GROUP):
            part = raw[g:g + GROUP]
            ps = [x[:, 0:128] for x in part]
            qs = [x[:, 128:256] for x in part]
            cols = [[pick_lane(p, base + r) for r in range(8)] for p in ps]
            for r in range(8):
                for i in range(len(part)):
                    c = cols[i][r]
                    inv = lax.rsqrt(jnp.broadcast_to(c[r:r + 1], (8, 128)))
                    cs = c * inv
                    prow = ps[i][r:r + 1] * inv
                    qrow = qs[i][r:r + 1] * inv
                    cz = jnp.where(sub > r, cs, 0.0)
                    ps[i] = jnp.where(sub == r, prow, ps[i] - cz * prow)
                    qs[i] = jnp.where(sub == r, qrow, qs[i] - cz * qrow)
                    for t in range(r + 1, 8):
                        cols[i][t] = cols[i][t] - cs * cs[t:t + 1]
            for i in range(len(part)):
                p = jnp.where(keep, ps[i], 0.0)
                full = jnp.concatenate([p, qs[i]], axis=1)
                rows.append(full)
                ph, pd, pe = split(jnp.where(below, p, 0.0))
                fh, fd, fe = split(full)
                left = jnp.concatenate([ph, ph, pd, ph, pe, pd], axis=0)
                right = jnp.concatenate([fh, fd, fh, fe, fh, fd], axis=0)
                leftT = left.T[top:].astype(jnp.bfloat16)
                prods.append(lax.dot_general(leftT, right.astype(jnp.bfloat16), (((1,), (0,)), ((), ())), preferred_element_type=jnp.float32))
        for m, full, prod in zip(mats, rows, prods):
            work[m, pl.ds(base, 8), :] = full
        for m, full, prod in zip(mats, rows, prods):
            work[m, top:128, :] = work[m, top:128, :] - prod

    for lo, hi in SEGS:
        def body(k, _, lo=lo):
            panel(k, lo * 8)
            return 0
        lax.fori_loop(lo, hi, body, 0)

def init_work(work, m, gram):
    r = lax.broadcasted_iota(jnp.int32, (128, 128), 0)
    c = lax.broadcasted_iota(jnp.int32, (128, 128), 1)
    work[m, :, 0:128] = gram
    work[m, :, 128:256] = jnp.where(r == c, 1.0, 0.0)


NODES = ((0, 1, 4), (2, 3, 5), (4, 5, 6), (7, 8, 9))


def times_transposed(x, y):
    return lax.dot_general(x, y, (((1,), (1,)), ((), ())), precision=precise, preferred_element_type=jnp.float32)


def write_outputs(work, rows, basis_ref, transfer_ref):
    for c in range(4):
        basis_ref[c] = times_transposed(rows[c], work[c, :, 128:256])
    last = lax.axis_index("dev") == lax.axis_size("dev") - 1
    for n, (left, right, parent) in enumerate(NODES):
        inverse = work[parent, :, 128:256]
        for half, child in enumerate((left, right)):
            made = times_transposed(work[child, :, 0:128], inverse)
            if n == 3:
                made = jnp.where(last, 0.0, made)
            transfer_ref[n, half * 128 : (half + 1) * 128, :] = made


def factor_kernel(gram_ref, rows_ref, basis_ref, transfer_ref, work):
    for m in range(10):
        init_work(work, m, gram_ref[m])
    factor_all(work, range(10))
    write_outputs(work, [rows_ref[c] for c in range(4)], basis_ref, transfer_ref)


def factor(grams, rows):
    vmem = pl.BlockSpec(memory_space=pltpu.VMEM)
    return pl.pallas_call(
        factor_kernel,
        out_shape=(
            jax.ShapeDtypeStruct((4, 64, 128), jnp.float32),
            jax.ShapeDtypeStruct((4, 256, 128), jnp.float32),
        ),
        in_specs=[vmem, vmem],
        out_specs=(vmem, vmem),
        scratch_shapes=[pltpu.VMEM((10, 128, 256), jnp.float32)],
        name="factor",
    )(grams, rows)


def split_up(value, dim, count):
    dims = value.shape
    pieces = value.reshape(*dims[:dim], count, dims[dim] // count, *dims[dim + 1 :])
    return jnp.moveaxis(pieces, dim, 0)


def sum_at_owner(value, axis, dim):
    pieces = split_up(value, dim, lax.axis_size(axis))
    arrived = lax.all_to_all(pieces, axis, split_axis=0, concat_axis=0, tiled=True)
    return arrived.sum(axis=0)


def copy_for_each(value, axis):
    copies = jnp.broadcast_to(value, (lax.axis_size(axis), *value.shape))
    return lax.all_to_all(copies, axis, split_axis=0, concat_axis=0, tiled=True)


def taken_together(value, axis):
    return copy_for_each(value, axis).sum(axis=0)


def swapped(value, axis, apart):
    mask = 2**apart
    pairs = [(source, source ^ mask) for source in range(lax.axis_size(axis))]
    return lax.ppermute(value, axis, pairs)


def on_device(omega, u_factor, v_factor, columns, ranks):
    n_local = u_factor.shape[1]
    n_blocks = u_factor.shape[2]
    leaf_rows = u_factor.shape[3]
    rank_width = u_factor.shape[4]
    probe_count = omega.shape[3]
    dev_count = lax.axis_size("dev")
    col_flat = columns[0, :, :, 0].reshape(n_local * n_blocks)
    v_flat = v_factor[0].reshape(n_local * n_blocks, leaf_rows, rank_width)
    whole_probe = lax.all_gather(omega, "dev", axis=1, tiled=True)[0]
    coeff = jnp.einsum("bik,bip->bkp", v_flat, whole_probe[col_flat], precision=fast)
    rank_mask = (
        jnp.arange(rank_width, dtype=jnp.int32)[None, None, :] < ranks[0][:, :, None]
    ).astype(jnp.float32)
    masked_rows = u_factor[0] * rank_mask[:, :, None, :]
    partial_sketch = jnp.einsum(
        "cbik,cbkp->cip",
        masked_rows,
        coeff.reshape(n_local, n_blocks, rank_width, probe_count),
        precision=fast,
    )
    own_rows = sum_at_owner(partial_sketch, "grp", 1)
    gram_matrix = taken_together(
        jnp.einsum("cip,ciq->cpq", own_rows, own_rows, precision=precise), "grp"
    )
    pair_gram = gram_matrix[0::2] + gram_matrix[1::2]
    top_gram = pair_gram[0] + pair_gram[1]
    device_index = lax.axis_index("dev")
    tree_bits = dev_count.bit_length() - 1
    keep_left = jnp.eye(probe_count, dtype=jnp.float32)
    keep_right = keep_left
    current = top_gram
    for depth_step in range(tree_bits):
        sibling = swapped(current, "dev", depth_step)
        is_left = device_index // 2**depth_step % 2 == 0
        left_gram = jnp.where(is_left, current, sibling)
        right_gram = jnp.where(is_left, sibling, current)
        owner = device_index % 2 ** (depth_step + 1) == 2**depth_step - 1
        keep_left = jnp.where(owner, left_gram, keep_left)
        keep_right = jnp.where(owner, right_gram, keep_right)
        current = left_gram + right_gram
    all_grams = jnp.concatenate(
        [
            gram_matrix,
            pair_gram,
            top_gram[None],
            keep_left[None],
            keep_right[None],
            (keep_left + keep_right)[None],
        ],
        axis=0,
    )
    return factor(all_grams, own_rows)


def solution(mesh):
    placed = (
        P("grp", "dev", None, None),
        P("grp", "dev", None, None, None),
        P("grp", "dev", None, None, None),
        P("grp", "dev", None, None),
        P("grp", "dev", None),
    )
    return jax.shard_map(
        on_device,
        mesh=mesh,
        in_specs=placed,
        out_specs=(P("dev", "grp", None), P("dev", None, None)),
        check_vma=False,
    )
```

```python
import functools
import jax
import jax.numpy as jnp
from jax import lax
from jax.experimental import pallas as pl
from jax.experimental.pallas import tpu as pltpu
from jax.sharding import PartitionSpec as P

precise = lax.Precision.HIGHEST
fast = lax.Precision.HIGH


GROUP = 5
SEGS = ((0, 4), (4, 8), (8, 12), (12, 16))

def pick_lane(x, lane):
    idx = jnp.full(x.shape, lane, jnp.int32)
    return jnp.take_along_axis(x, idx, axis=1)

def factor_all(work, mats):
    sub = lax.broadcasted_iota(jnp.int32, (8, 128), 0)
    lane = lax.broadcasted_iota(jnp.int32, (8, 128), 1)

    def split(x):
        h = x.astype(jnp.bfloat16).astype(jnp.float32)
        rest = x - h
        d = rest.astype(jnp.bfloat16).astype(jnp.float32)
        return h, d, rest - d

    def panel(k, top):
        base = pl.multiple_of(k * 8, 8)
        raw = [work[m, pl.ds(base, 8), :] for m in mats]
        keep = lane >= base + sub
        below = lane >= base + 8
        prods = []
        rows = []
        for g in range(0, len(mats), GROUP):
            part = raw[g:g + GROUP]
            ps = [x[:, 0:128] for x in part]
            qs = [x[:, 128:256] for x in part]
            cols = [[pick_lane(p, base + r) for r in range(8)] for p in ps]
            for r in range(8):
                for i in range(len(part)):
                    c = cols[i][r]
                    inv = lax.rsqrt(jnp.broadcast_to(c[r:r + 1], (8, 128)))
                    cs = c * inv
                    prow = ps[i][r:r + 1] * inv
                    qrow = qs[i][r:r + 1] * inv
                    cz = jnp.where(sub > r, cs, 0.0)
                    ps[i] = jnp.where(sub == r, prow, ps[i] - cz * prow)
                    qs[i] = jnp.where(sub == r, qrow, qs[i] - cz * qrow)
                    for t in range(r + 1, 8):
                        cols[i][t] = cols[i][t] - cs * cs[t:t + 1]
            for i in range(len(part)):
                p = jnp.where(keep, ps[i], 0.0)
                full = jnp.concatenate([p, qs[i]], axis=1)
                rows.append(full)
                ph, pd, pe = split(jnp.where(below, p, 0.0))
                fh, fd, fe = split(full)
                left = jnp.concatenate([ph, ph, pd, ph, pe, pd], axis=0)
                right = jnp.concatenate([fh, fd, fh, fe, fh, fd], axis=0)
                leftT = left.T[top:].astype(jnp.bfloat16)
                prods.append(lax.dot_general(leftT, right.astype(jnp.bfloat16), (((1,), (0,)), ((), ())), preferred_element_type=jnp.float32))
        for m, full, prod in zip(mats, rows, prods):
            work[m, pl.ds(base, 8), :] = full
        for m, full, prod in zip(mats, rows, prods):
            work[m, top:128, :] = work[m, top:128, :] - prod

    for lo, hi in SEGS:
        def body(k, _, lo=lo):
            panel(k, lo * 8)
            return 0
        lax.fori_loop(lo, hi, body, 0)

def init_work(work, m, gram):
    r = lax.broadcasted_iota(jnp.int32, (128, 128), 0)
    c = lax.broadcasted_iota(jnp.int32, (128, 128), 1)
    work[m, :, 0:128] = gram
    work[m, :, 128:256] = jnp.where(r == c, 1.0, 0.0)


NODES = ((0, 1, 4), (2, 3, 5), (4, 5, 6), (7, 8, 9))


def times_transposed(x, y):
    return lax.dot_general(x, y, (((1,), (1,)), ((), ())), precision=precise, preferred_element_type=jnp.float32)


def write_outputs(work, rows, basis_ref, transfer_ref):
    for c in range(4):
        basis_ref[c] = times_transposed(rows[c], work[c, :, 128:256])
    last = lax.axis_index("dev") == lax.axis_size("dev") - 1
    for n, (left, right, parent) in enumerate(NODES):
        inverse = work[parent, :, 128:256]
        for half, child in enumerate((left, right)):
            made = times_transposed(work[child, :, 0:128], inverse)
            if n == 3:
                made = jnp.where(last, 0.0, made)
            transfer_ref[n, half * 128 : (half + 1) * 128, :] = made


def factor_kernel(gram_ref, rows_ref, basis_ref, transfer_ref, work):
    for m in range(10):
        init_work(work, m, gram_ref[m])
    factor_all(work, range(10))
    write_outputs(work, [rows_ref[c] for c in range(4)], basis_ref, transfer_ref)


def factor(grams, rows):
    vmem = pl.BlockSpec(memory_space=pltpu.VMEM)
    return pl.pallas_call(
        factor_kernel,
        out_shape=(
            jax.ShapeDtypeStruct((4, 64, 128), jnp.float32),
            jax.ShapeDtypeStruct((4, 256, 128), jnp.float32),
        ),
        in_specs=[vmem, vmem],
        out_specs=(vmem, vmem),
        scratch_shapes=[pltpu.VMEM((10, 128, 256), jnp.float32)],
        name="factor",
    )(grams, rows)


RIGHT, LEFT, DOWN, UP, ACROSS = range(5)


def split_two(x):
    high = x.astype(jnp.bfloat16)
    low = (x - high.astype(jnp.float32)).astype(jnp.bfloat16)
    return high, low


def bf16_dot(x, y):
    return lax.dot_general(x, y, (((1,), (0,)), ((), ())), preferred_element_type=jnp.float32)


def gather_kernel(
    slot_ref, place_ref, rank_ref, omega_ref, u_ref, v_ref, sketch_ref,
    probe, u_all, v_all, u_high, u_low, coeff, weights, load_sem, send_sem, recv_sem,
):
    me = lax.axis_index("dev")
    core = me % 2
    x_at = me // 2 % 4
    y_at = me // 8
    partner = me + 1 - 2 * core

    def device(dy, dx):
        return ((y_at + dy) % 4 * 4 + (x_at + dx) % 4) * 2 + core

    targets = (device(0, 1), device(0, 3), device(1, 0), device(3, 0), partner)
    own = pltpu.make_async_copy(omega_ref, probe.at[pl.ds(me * 4, 4)], load_sem.at[0])
    own.start()
    loads = [
        pltpu.make_async_copy(v_ref, v_all, load_sem.at[1]),
        pltpu.make_async_copy(u_ref, u_all, load_sem.at[2]),
    ]
    for load in loads:
        load.start()
    barrier = pltpu.get_barrier_semaphore()
    for target in targets:
        pl.semaphore_signal(barrier, inc=1, device_id={"dev": target}, device_id_type=pl.DeviceIdType.MESH)
    pl.semaphore_wait(barrier, 5)
    own.wait()

    def move(cluster, way):
        return pltpu.make_async_remote_copy(
            src_ref=probe.at[cluster],
            dst_ref=probe.at[cluster],
            send_sem=send_sem.at[way],
            recv_sem=recv_sem.at[cluster],
            device_id={"dev": targets[way]},
            device_id_type=pl.DeviceIdType.MESH,
        )

    def await_cluster(cluster):
        move(cluster, RIGHT).wait_recv()

    def make_coeff(cluster):
        wide = jnp.concatenate(split_two(probe[cluster]), axis=1)
        rows = jnp.concatenate([v_all[slot_ref[cluster * 3 + t]] for t in range(3)], axis=0)
        high, low = split_two(rows)
        both = bf16_dot(high, wide)
        made = both[:, 0:128] + both[:, 128:256] + bf16_dot(low, wide[:, 0:128])
        packed = jnp.concatenate(split_two(made), axis=1)
        for t in range(3):
            coeff[cluster * 3 + t] = packed[t * 32 : t * 32 + 32]

    rank_row = lax.broadcasted_iota(jnp.int32, (32, 256), 0)

    def turn_rows(chunk):
        pieces = [
            jnp.where(rank_row < rank_ref[chunk * 8 + e], u_all[chunk * 8 + e], 0.0) for e in range(8)
        ]
        high, low = split_two(jnp.concatenate(pieces, axis=0).T)
        leaf = chunk // 10
        where = pl.ds(pl.multiple_of(chunk % 10 * 256, 256), 256)
        u_high[leaf, :, where] = high
        u_low[leaf, :, where] = low

    def step(dy, dx, j, before, first=False, chunk=None):
        along_x = device(dy, dx) * 4 + j
        along_y = device(dx, dy) * 4 + j + 2
        flips = ((along_x, (RIGHT, LEFT, DOWN, UP)), (along_y, (DOWN, UP, RIGHT, LEFT)))
        for cluster, (ahead, back, out, home) in flips:
            if not first:
                await_cluster(cluster)
            ways = []
            if isinstance(dy, int) and dy == 0:
                if first:
                    ways += [ahead, back]
                elif dx == 3 and j == 0:
                    ways += [ahead]
                elif dx == 1 and j == 1:
                    ways += [back]
                ways += [out, home]
            elif dy == 3 and j == 0:
                ways += [out]
            elif dy == 1 and j == 1:
                ways += [home]
            for way in ways + [ACROSS]:
                move(cluster, way).start()
        now = [along_x, along_y]
        work = list(now)
        if before is not None:
            for cluster in before:
                await_cluster(cluster)
                work.append(cluster)
        if first and j == 0:
            loads[0].wait()
        for cluster in work:
            make_coeff(cluster)
        if chunk is not None:
            turn_rows(chunk)
            turn_rows(chunk + 1)
        shift = 4 - 8 * core
        return [c + shift for c in now]

    late = step(0, 0, 0, None, first=True)
    late = step(0, 0, 1, late, first=True)
    loads[1].wait()

    def turn_some(chunk, carry):
        turn_rows(chunk)
        return carry

    lax.fori_loop(0, 8, turn_some, 0)
    for dx, j in ((3, 0), (1, 1), (3, 1), (1, 0), (2, 0), (2, 1)):
        late = step(0, dx, j, late)

    def far(q):
        return jnp.where(q == 0, 0, jnp.where(q == 1, 3, q - 1))

    def cross(q, late):
        for s, (dy, j) in enumerate(((3, 0), (1, 1), (3, 1), (1, 0))):
            late = step(dy, far(q), j, late, chunk=8 + q * 8 + s * 2)
        return tuple(late)

    def end(q, late):
        for j in range(2):
            late = step(2, far(q), j, late)
        return tuple(late)

    late = lax.fori_loop(0, 4, cross, tuple(late))
    late = lax.fori_loop(0, 4, end, late)
    for cluster in late:
        await_cluster(cluster)
    for cluster in late:
        make_coeff(cluster)

    def sketch_leaf(leaf, carry):
        for b in range(80):
            weights[b * 32 : b * 32 + 32, :] = coeff[place_ref[leaf * 80 + b]]
        both = bf16_dot(u_high[leaf], weights[...])
        sketch_ref[leaf] = both[:, 0:128] + both[:, 128:256] + bf16_dot(u_low[leaf], weights[:, 0:128])
        return carry

    lax.fori_loop(0, 4, sketch_leaf, 0)
    for way in range(4):
        span = pl.ds(0, 15)
        pltpu.make_async_remote_copy(
            src_ref=probe.at[span], dst_ref=probe.at[span], send_sem=send_sem.at[way], recv_sem=recv_sem.at[0],
            device_id={"dev": targets[way]}, device_id_type=pl.DeviceIdType.MESH,
        ).wait_send()
    span = pl.ds(0, 64)
    pltpu.make_async_remote_copy(
        src_ref=probe.at[span], dst_ref=probe.at[span], send_sem=send_sem.at[ACROSS], recv_sem=recv_sem.at[0],
        device_id={"dev": partner}, device_id_type=pl.DeviceIdType.MESH,
    ).wait_send()


def sketch_of_group(slots, places, ranks, omega, u_rows, v_rows):
    smem = pl.BlockSpec(memory_space=pltpu.SMEM)
    anywhere = pl.BlockSpec(memory_space=pl.ANY)
    return pl.pallas_call(
        gather_kernel,
        out_shape=jax.ShapeDtypeStruct((4, 256, 128), jnp.float32),
        in_specs=[smem, smem, smem, anywhere, anywhere, anywhere],
        out_specs=pl.BlockSpec(memory_space=pltpu.VMEM),
        scratch_shapes=[
            pltpu.VMEM((128, 256, 128), jnp.float32),
            pltpu.VMEM((320, 32, 256), jnp.float32),
            pltpu.VMEM((320, 32, 256), jnp.float32),
            pltpu.VMEM((4, 256, 2560), jnp.bfloat16),
            pltpu.VMEM((4, 256, 2560), jnp.bfloat16),
            pltpu.VMEM((384, 32, 256), jnp.bfloat16),
            pltpu.VMEM((2560, 256), jnp.bfloat16),
            pltpu.SemaphoreType.DMA((3,)),
            pltpu.SemaphoreType.DMA((5,)),
            pltpu.SemaphoreType.DMA((128,)),
        ],
        compiler_params=pltpu.CompilerParams(
            collective_id=0, has_side_effects=True, vmem_limit_bytes=62 * 2**20
        ),
        name="gather",
    )(slots, places, ranks, omega, u_rows, v_rows)


def sort_blocks(columns):
    named = columns[0, :, :, 0].reshape(320)
    number = jnp.arange(320, dtype=jnp.int32)
    same = named[:, None] == named[None, :]
    turn = jnp.sum((same & (number[None, :] < number[:, None])).astype(jnp.int32), axis=1)
    places = named * 3 + turn
    slots = jnp.arange(384, dtype=jnp.int32)
    hit = places[None, :] == slots[:, None]
    return jnp.sum(jnp.where(hit, number[None, :], 0), axis=1), places


def split_up(value, dim, count):
    dims = value.shape
    pieces = value.reshape(*dims[:dim], count, dims[dim] // count, *dims[dim + 1 :])
    return jnp.moveaxis(pieces, dim, 0)


def sum_at_owner(value, axis, dim):
    pieces = split_up(value, dim, lax.axis_size(axis))
    arrived = lax.all_to_all(pieces, axis, split_axis=0, concat_axis=0, tiled=True)
    return arrived.sum(axis=0)


def copy_for_each(value, axis):
    copies = jnp.broadcast_to(value, (lax.axis_size(axis), *value.shape))
    return lax.all_to_all(copies, axis, split_axis=0, concat_axis=0, tiled=True)


def taken_together(value, axis):
    return copy_for_each(value, axis).sum(axis=0)


def swapped(value, axis, apart):
    mask = 2**apart
    pairs = [(source, source ^ mask) for source in range(lax.axis_size(axis))]
    return lax.ppermute(value, axis, pairs)


def on_device(omega, u_factor, v_factor, columns, ranks):
    probe_count = omega.shape[3]
    dev_count = lax.axis_size("dev")
    slots, places = sort_blocks(columns)
    u_rows = jnp.swapaxes(u_factor, 3, 4).reshape(320, 32, 256)
    v_rows = jnp.swapaxes(v_factor, 3, 4).reshape(320, 32, 256)
    partial_sketch = sketch_of_group(slots, places, ranks.reshape(320), omega[0], u_rows, v_rows)
    own_rows = sum_at_owner(partial_sketch, "grp", 1)
    gram_matrix = taken_together(
        jnp.einsum("cip,ciq->cpq", own_rows, own_rows, precision=precise), "grp"
    )
    pair_gram = gram_matrix[0::2] + gram_matrix[1::2]
    top_gram = pair_gram[0] + pair_gram[1]
    device_index = lax.axis_index("dev")
    tree_bits = dev_count.bit_length() - 1
    keep_left = jnp.eye(probe_count, dtype=jnp.float32)
    keep_right = keep_left
    current = top_gram
    for depth_step in range(tree_bits):
        sibling = swapped(current, "dev", depth_step)
        is_left = device_index // 2**depth_step % 2 == 0
        left_gram = jnp.where(is_left, current, sibling)
        right_gram = jnp.where(is_left, sibling, current)
        owner = device_index % 2 ** (depth_step + 1) == 2**depth_step - 1
        keep_left = jnp.where(owner, left_gram, keep_left)
        keep_right = jnp.where(owner, right_gram, keep_right)
        current = left_gram + right_gram
    all_grams = jnp.concatenate(
        [
            gram_matrix,
            pair_gram,
            top_gram[None],
            keep_left[None],
            keep_right[None],
            (keep_left + keep_right)[None],
        ],
        axis=0,
    )
    return factor(all_grams, own_rows)


def solution(mesh):
    placed = (
        P("grp", "dev", None, None),
        P("grp", "dev", None, None, None),
        P("grp", "dev", None, None, None),
        P("grp", "dev", None, None),
        P("grp", "dev", None),
    )
    return jax.shard_map(
        on_device,
        mesh=mesh,
        in_specs=placed,
        out_specs=(P("dev", "grp", None), P("dev", None, None)),
        check_vma=False,
    )
```

```python
import functools
import jax
import jax.numpy as jnp
from jax import lax
from jax.experimental import pallas as pl
from jax.experimental.pallas import tpu as pltpu
from jax.sharding import PartitionSpec as P

precise = lax.Precision.HIGHEST


GROUP = 5
SEGS = ((0, 4), (4, 8), (8, 12), (12, 16))

def pick_lane(x, lane):
    idx = jnp.full(x.shape, lane, jnp.int32)
    return jnp.take_along_axis(x, idx, axis=1)

def factor_all(work, mats):
    sub = lax.broadcasted_iota(jnp.int32, (8, 128), 0)
    lane = lax.broadcasted_iota(jnp.int32, (8, 128), 1)

    def split(x):
        h = x.astype(jnp.bfloat16).astype(jnp.float32)
        rest = x - h
        d = rest.astype(jnp.bfloat16).astype(jnp.float32)
        return h, d, rest - d

    def panel(k, top):
        base = pl.multiple_of(k * 8, 8)
        raw = [work[m, pl.ds(base, 8), :] for m in mats]
        keep = lane >= base + sub
        below = lane >= base + 8
        prods = []
        rows = []
        for g in range(0, len(mats), GROUP):
            part = raw[g:g + GROUP]
            ps = [x[:, 0:128] for x in part]
            qs = [x[:, 128:256] for x in part]
            cols = [[pick_lane(p, base + r) for r in range(8)] for p in ps]
            for r in range(8):
                for i in range(len(part)):
                    c = cols[i][r]
                    inv = lax.rsqrt(jnp.broadcast_to(c[r:r + 1], (8, 128)))
                    cs = c * inv
                    prow = ps[i][r:r + 1] * inv
                    qrow = qs[i][r:r + 1] * inv
                    cz = jnp.where(sub > r, cs, 0.0)
                    ps[i] = jnp.where(sub == r, prow, ps[i] - cz * prow)
                    qs[i] = jnp.where(sub == r, qrow, qs[i] - cz * qrow)
                    for t in range(r + 1, 8):
                        cols[i][t] = cols[i][t] - cs * cs[t:t + 1]
            for i in range(len(part)):
                p = jnp.where(keep, ps[i], 0.0)
                full = jnp.concatenate([p, qs[i]], axis=1)
                rows.append(full)
                ph, pd, pe = split(jnp.where(below, p, 0.0))
                fh, fd, fe = split(full)
                left = jnp.concatenate([ph, ph, pd, ph, pe, pd], axis=0)
                right = jnp.concatenate([fh, fd, fh, fe, fh, fd], axis=0)
                leftT = left.T[top:].astype(jnp.bfloat16)
                prods.append(lax.dot_general(leftT, right.astype(jnp.bfloat16), (((1,), (0,)), ((), ())), preferred_element_type=jnp.float32))
        for m, full, prod in zip(mats, rows, prods):
            work[m, pl.ds(base, 8), :] = full
        for m, full, prod in zip(mats, rows, prods):
            work[m, top:128, :] = work[m, top:128, :] - prod

    for lo, hi in SEGS:
        def body(k, _, lo=lo):
            panel(k, lo * 8)
            return 0
        lax.fori_loop(lo, hi, body, 0)

def init_work(work, m, gram):
    r = lax.broadcasted_iota(jnp.int32, (128, 128), 0)
    c = lax.broadcasted_iota(jnp.int32, (128, 128), 1)
    work[m, :, 0:128] = gram
    work[m, :, 128:256] = jnp.where(r == c, 1.0, 0.0)


NODES = ((0, 1, 4), (2, 3, 5), (4, 5, 6), (7, 8, 9))


def times_transposed(x, y):
    return lax.dot_general(x, y, (((1,), (1,)), ((), ())), precision=precise, preferred_element_type=jnp.float32)


def write_outputs(work, rows, basis_ref, transfer_ref):
    for c in range(4):
        basis_ref[c] = times_transposed(rows[c], work[c, :, 128:256])
    last = lax.axis_index("dev") == lax.axis_size("dev") - 1
    for n, (left, right, parent) in enumerate(NODES):
        inverse = work[parent, :, 128:256]
        for half, child in enumerate((left, right)):
            made = times_transposed(work[child, :, 0:128], inverse)
            if n == 3:
                made = jnp.where(last, 0.0, made)
            transfer_ref[n, half * 128 : (half + 1) * 128, :] = made


def factor_kernel(gram_ref, rows_ref, basis_ref, transfer_ref, work):
    for m in range(10):
        init_work(work, m, gram_ref[m])
    factor_all(work, range(10))
    write_outputs(work, [rows_ref[c] for c in range(4)], basis_ref, transfer_ref)


def factor(grams, rows):
    vmem = pl.BlockSpec(memory_space=pltpu.VMEM)
    return pl.pallas_call(
        factor_kernel,
        out_shape=(
            jax.ShapeDtypeStruct((4, 64, 128), jnp.float32),
            jax.ShapeDtypeStruct((4, 256, 128), jnp.float32),
        ),
        in_specs=[vmem, vmem],
        out_specs=(vmem, vmem),
        scratch_shapes=[pltpu.VMEM((10, 128, 256), jnp.float32)],
        name="factor",
    )(grams, rows)


RIGHT, LEFT, DOWN, UP, ACROSS = range(5)


def split_two(x):
    high = x.astype(jnp.bfloat16)
    low = (x - high.astype(jnp.float32)).astype(jnp.bfloat16)
    return high, low


def bf16_dot(x, y):
    return lax.dot_general(x, y, (((1,), (0,)), ((), ())), preferred_element_type=jnp.float32)


def gather_kernel(
    slot_ref, place_ref, rank_ref, omega_ref, u_ref, v_ref, gram_ref, rows_ref,
    probe, u_all, v_all, u_high, u_low, coeff, weights,
    sketch, relay, parts, whole, leaf_gram, leaf_rows, top_gram, tree, eights,
    load_sem, send_sem, recv_sem, out_sem, in_sem,
):
    me = lax.axis_index("dev")
    core = me % 2
    x_at = me // 2 % 4
    y_at = me // 8
    partner = me + 1 - 2 * core

    def device(dy, dx):
        return ((y_at + dy) % 4 * 4 + (x_at + dx) % 4) * 2 + core

    targets = (device(0, 1), device(0, 3), device(1, 0), device(3, 0), partner)
    own = pltpu.make_async_copy(omega_ref, probe.at[pl.ds(me * 4, 4)], load_sem.at[0])
    own.start()
    loads = [
        pltpu.make_async_copy(v_ref, v_all, load_sem.at[1]),
        pltpu.make_async_copy(u_ref, u_all, load_sem.at[2]),
    ]
    for load in loads:
        load.start()
    z = lax.axis_index("grp")
    e = me % 8
    barrier = pltpu.get_barrier_semaphore()
    peers = [{"dev": me // 8 * 8 + (e + n) % 8} for n in range(1, 8)]
    peers += [{"dev": (me + 8 * n) % 32} for n in range(1, 4)]
    peers += [{"grp": (z + n) % 4} for n in range(1, 4)]
    for peer in peers:
        pl.semaphore_signal(barrier, inc=1, device_id=peer, device_id_type=pl.DeviceIdType.MESH)
    pl.semaphore_wait(barrier, 13)
    own.wait()

    def move(cluster, way):
        return pltpu.make_async_remote_copy(
            src_ref=probe.at[cluster],
            dst_ref=probe.at[cluster],
            send_sem=send_sem.at[way],
            recv_sem=recv_sem.at[cluster],
            device_id={"dev": targets[way]},
            device_id_type=pl.DeviceIdType.MESH,
        )

    def await_cluster(cluster):
        move(cluster, RIGHT).wait_recv()

    def make_coeff(cluster):
        wide = jnp.concatenate(split_two(probe[cluster]), axis=1)
        rows = jnp.concatenate([v_all[slot_ref[cluster * 3 + t]] for t in range(3)], axis=0)
        high, low = split_two(rows)
        both = bf16_dot(high, wide)
        made = both[:, 0:128] + both[:, 128:256] + bf16_dot(low, wide[:, 0:128])
        packed = jnp.concatenate(split_two(made), axis=1)
        for t in range(3):
            coeff[cluster * 3 + t] = packed[t * 32 : t * 32 + 32]

    rank_row = lax.broadcasted_iota(jnp.int32, (32, 256), 0)

    def turn_rows(chunk):
        pieces = [
            jnp.where(rank_row < rank_ref[chunk * 8 + e], u_all[chunk * 8 + e], 0.0) for e in range(8)
        ]
        high, low = split_two(jnp.concatenate(pieces, axis=0).T)
        leaf = chunk // 10
        where = pl.ds(pl.multiple_of(chunk % 10 * 256, 256), 256)
        u_high[leaf, :, where] = high
        u_low[leaf, :, where] = low

    def step(dy, dx, j, before, first=False, chunk=None):
        along_x = device(dy, dx) * 4 + j
        along_y = device(dx, dy) * 4 + j + 2
        flips = ((along_x, (RIGHT, LEFT, DOWN, UP)), (along_y, (DOWN, UP, RIGHT, LEFT)))
        for cluster, (ahead, back, out, home) in flips:
            if not first:
                await_cluster(cluster)
            ways = []
            if isinstance(dy, int) and dy == 0:
                if first:
                    ways += [ahead, back]
                elif dx == 3 and j == 0:
                    ways += [ahead]
                elif dx == 1 and j == 1:
                    ways += [back]
                ways += [out, home]
            elif dy == 3 and j == 0:
                ways += [out]
            elif dy == 1 and j == 1:
                ways += [home]
            for way in ways + [ACROSS]:
                move(cluster, way).start()
        now = [along_x, along_y]
        work = list(now)
        if before is not None:
            for cluster in before:
                await_cluster(cluster)
                work.append(cluster)
        if first and j == 0:
            loads[0].wait()
        for cluster in work:
            make_coeff(cluster)
        if chunk is not None:
            turn_rows(chunk)
            turn_rows(chunk + 1)
        shift = 4 - 8 * core
        return [c + shift for c in now]

    late = step(0, 0, 0, None, first=True)
    late = step(0, 0, 1, late, first=True)
    loads[1].wait()

    def turn_some(chunk, carry):
        turn_rows(chunk)
        return carry

    lax.fori_loop(0, 8, turn_some, 0)
    for dx, j in ((3, 0), (1, 1), (3, 1), (1, 0), (2, 0), (2, 1)):
        late = step(0, dx, j, late)

    def far(q):
        return jnp.where(q == 0, 0, jnp.where(q == 1, 3, q - 1))

    def cross(q, late):
        for s, (dy, j) in enumerate(((3, 0), (1, 1), (3, 1), (1, 0))):
            late = step(dy, far(q), j, late, chunk=8 + q * 8 + s * 2)
        return tuple(late)

    def end(q, late):
        for j in range(2):
            late = step(2, far(q), j, late)
        return tuple(late)

    late = lax.fori_loop(0, 4, cross, tuple(late))
    late = lax.fori_loop(0, 4, end, late)
    for cluster in late:
        await_cluster(cluster)
    for cluster in late:
        make_coeff(cluster)

    def sketch_leaf(leaf):
        for b in range(80):
            weights[b * 32 : b * 32 + 32, :] = coeff[place_ref[leaf * 80 + b]]
        both = bf16_dot(u_high[leaf], weights[...])
        sketch[leaf] = both[:, 0:128] + both[:, 128:256] + bf16_dot(u_low[leaf], weights[:, 0:128])

    def send(source, target, out, arrival, peer):
        return pltpu.make_async_remote_copy(
            src_ref=source,
            dst_ref=target,
            send_sem=out_sem.at[out],
            recv_sem=in_sem.at[arrival],
            device_id=peer,
            device_id_type=pl.DeviceIdType.MESH,
        )

    top, bottom = pl.ds(0, 128), pl.ds(128, 128)
    after, across_z, before = [(z + n) % 4 for n in (1, 2, 3)]
    to_after, to_across, to_before = [{"grp": n} for n in (after, across_z, before)]
    far_out = send(sketch.at[across_z, top], relay.at[0], 0, 0, to_after)
    far_home = send(sketch.at[across_z, bottom], relay.at[1], 1, 1, to_before)
    near_out = send(sketch.at[after, bottom], parts.at[0], 2, 2, to_after)
    near_home = send(sketch.at[before, top], parts.at[1], 3, 3, to_before)
    joint_out = send(sketch.at[after, top], parts.at[2], 4, 4, to_after)
    joint_home = send(sketch.at[before, bottom], parts.at[3], 5, 5, to_before)

    def leaf_step(n, carry):
        sketch_leaf((z + jnp.where(n == 0, 2, jnp.where(n == 1, 1, jnp.where(n == 2, 3, 0)))) % 4)

        @pl.when(n == 0)
        def _():
            far_out.start()
            far_home.start()

        @pl.when(n == 1)
        def _():
            near_out.start()

        @pl.when(n == 2)
        def _():
            near_home.start()

        return carry

    lax.fori_loop(0, 4, leaf_step, 0)
    far_out.wait_recv()
    sketch[after, 0:128] = sketch[after, 0:128] + relay[0]
    joint_out.start()
    far_home.wait_recv()
    sketch[before, 128:256] = sketch[before, 128:256] + relay[1]
    joint_home.start()
    near_out.wait_recv()
    near_home.wait_recv()
    joint_out.wait_recv()
    whole[0:128] = sketch[z, 0:128] + parts[1] + parts[2]
    joint_home.wait_recv()
    whole[128:256] = sketch[z, 128:256] + parts[0] + parts[3]
    flat = whole[...]
    leaf_gram[z] = lax.dot_general(
        flat.T, flat, (((1,), (0,)), ((), ())), precision=precise, preferred_element_type=jnp.float32
    )
    others = ((2, across_z, to_across), (1, after, to_after), (3, before, to_before))
    gram_sends = [send(leaf_gram.at[z], leaf_gram.at[z], 5 + n, 6 + z, peer) for n, _, peer in others]
    row_sends = [
        send(whole.at[pl.ds(pl.multiple_of(there * 64, 64), 64)], leaf_rows.at[z], 8 + n, 10 + z, peer)
        for n, there, peer in others
    ]
    for copy in gram_sends + row_sends:
        copy.start()
    leaf_rows[z] = whole[pl.ds(pl.multiple_of(z * 64, 64), 64)]
    for _, there, peer in others:
        send(leaf_gram.at[there], leaf_gram.at[there], 6, 6 + there, peer).wait_recv()
    first_pair = leaf_gram[0] + leaf_gram[1]
    second_pair = leaf_gram[2] + leaf_gram[3]
    own_top = first_pair + second_pair
    top_gram[...] = own_top

    def tree_send(slot, target):
        return send(top_gram, tree.at[e], 12 + slot, 14 + e, {"dev": me // 8 * 8 + target})

    tree_sends = (
        (e != 7, tree_send(0, 7)),
        (e != 3, tree_send(1, 3)),
        (e % 4 != 1, tree_send(2, e // 4 * 4 + 1)),
        (e % 2 == 1, tree_send(3, e - 1)),
    )
    for needed, copy in tree_sends:
        pl.when(needed)(copy.start)
    for c in range(4):
        gram_ref[c] = leaf_gram[c]
    gram_ref[4] = first_pair
    gram_ref[5] = second_pair
    gram_ref[6] = own_top

    def arrived(slot):
        send(top_gram, tree.at[slot], 12, 14 + slot, to_after).wait_recv()
        return tree[slot]

    def keep(left, right):
        gram_ref[7] = left
        gram_ref[8] = right
        gram_ref[9] = left + right

    @pl.when(e % 2 == 0)
    def _():
        keep(own_top, arrived(e + 1))

    @pl.when(e % 4 == 1)
    def _():
        keep(arrived(e - 1) + own_top, arrived(e + 1) + arrived(e + 2))

    @pl.when(e == 3)
    def _():
        left = arrived(0) + arrived(1) + (arrived(2) + own_top)
        keep(left, arrived(4) + arrived(5) + (arrived(6) + arrived(7)))

    def eight_send(slot, row):
        return send(top_gram, eights.at[y_at], 16 + slot, 22 + y_at, {"dev": row * 8 + 7})

    eight_sends = (
        (e * 4 + y_at == 28, eight_send(0, 1)),
        (e * 4 + y_at == 29, eight_send(0, 0)),
        (e * 4 + y_at == 30, eight_send(0, 1)),
        (e * 4 + y_at == 31, eight_send(0, 1)),
        (e * 4 + y_at == 31, eight_send(1, 2)),
    )

    @pl.when(e == 7)
    def _():
        pairs = [arrived(0) + arrived(1), arrived(2) + arrived(3), arrived(4) + arrived(5), arrived(6) + own_top]
        for needed, copy in tree_sends:
            pl.when(needed)(copy.wait_send)
        eight = (pairs[0] + pairs[1]) + (pairs[2] + pairs[3])
        top_gram[...] = eight
        for needed, copy in eight_sends:
            pl.when(needed)(copy.start)

        def landed(row):
            send(top_gram, eights.at[row], 16, 22 + row, to_after).wait_recv()
            return eights[row]

        @pl.when(y_at == 0)
        def _():
            keep(eight, landed(1))

        @pl.when(y_at == 1)
        def _():
            keep(landed(0) + eight, landed(2) + landed(3))

        @pl.when(y_at == 2)
        def _():
            keep(eight, landed(3))

        @pl.when(y_at == 3)
        def _():
            keep(eight, eight)

        for needed, copy in eight_sends:
            pl.when(needed)(copy.wait_send)

    @pl.when(e != 7)
    def _():
        for needed, copy in tree_sends:
            pl.when(needed)(copy.wait_send)

    for _, there, peer in others:
        send(leaf_rows.at[there], leaf_rows.at[there], 9, 10 + there, peer).wait_recv()
    rows_ref[...] = leaf_rows[...]
    for copy in [far_out, far_home, near_out, near_home, joint_out, joint_home] + gram_sends + row_sends:
        copy.wait_send()
    for way in range(4):
        span = pl.ds(0, 15)
        pltpu.make_async_remote_copy(
            src_ref=probe.at[span], dst_ref=probe.at[span], send_sem=send_sem.at[way], recv_sem=recv_sem.at[0],
            device_id={"dev": targets[way]}, device_id_type=pl.DeviceIdType.MESH,
        ).wait_send()
    span = pl.ds(0, 64)
    pltpu.make_async_remote_copy(
        src_ref=probe.at[span], dst_ref=probe.at[span], send_sem=send_sem.at[ACROSS], recv_sem=recv_sem.at[0],
        device_id={"dev": partner}, device_id_type=pl.DeviceIdType.MESH,
    ).wait_send()


def sum_sketches(slots, places, ranks, omega, u_rows, v_rows):
    smem = pl.BlockSpec(memory_space=pltpu.SMEM)
    anywhere = pl.BlockSpec(memory_space=pl.ANY)
    return pl.pallas_call(
        gather_kernel,
        out_shape=(
            jax.ShapeDtypeStruct((10, 128, 128), jnp.float32),
            jax.ShapeDtypeStruct((4, 64, 128), jnp.float32),
        ),
        in_specs=[smem, smem, smem, anywhere, anywhere, anywhere],
        out_specs=(pl.BlockSpec(memory_space=pltpu.VMEM), pl.BlockSpec(memory_space=pltpu.VMEM)),
        scratch_shapes=[
            pltpu.VMEM((128, 256, 128), jnp.float32),
            pltpu.VMEM((320, 32, 256), jnp.float32),
            pltpu.VMEM((320, 32, 256), jnp.float32),
            pltpu.VMEM((4, 256, 2560), jnp.bfloat16),
            pltpu.VMEM((4, 256, 2560), jnp.bfloat16),
            pltpu.VMEM((384, 32, 256), jnp.bfloat16),
            pltpu.VMEM((2560, 256), jnp.bfloat16),
            pltpu.VMEM((4, 256, 128), jnp.float32),
            pltpu.VMEM((2, 128, 128), jnp.float32),
            pltpu.VMEM((4, 128, 128), jnp.float32),
            pltpu.VMEM((256, 128), jnp.float32),
            pltpu.VMEM((4, 128, 128), jnp.float32),
            pltpu.VMEM((4, 64, 128), jnp.float32),
            pltpu.VMEM((128, 128), jnp.float32),
            pltpu.VMEM((8, 128, 128), jnp.float32),
            pltpu.VMEM((4, 128, 128), jnp.float32),
            pltpu.SemaphoreType.DMA((3,)),
            pltpu.SemaphoreType.DMA((5,)),
            pltpu.SemaphoreType.DMA((128,)),
            pltpu.SemaphoreType.DMA((18,)),
            pltpu.SemaphoreType.DMA((26,)),
        ],
        compiler_params=pltpu.CompilerParams(
            collective_id=0, has_side_effects=True, vmem_limit_bytes=62 * 2**20
        ),
        name="gather",
    )(slots, places, ranks, omega, u_rows, v_rows)


def sort_blocks(columns):
    named = columns[0, :, :, 0].reshape(320)
    number = jnp.arange(320, dtype=jnp.int32)
    same = named[:, None] == named[None, :]
    turn = jnp.sum((same & (number[None, :] < number[:, None])).astype(jnp.int32), axis=1)
    places = named * 3 + turn
    slots = jnp.arange(384, dtype=jnp.int32)
    hit = places[None, :] == slots[:, None]
    return jnp.sum(jnp.where(hit, number[None, :], 0), axis=1), places


def on_device(omega, u_factor, v_factor, columns, ranks):
    slots, places = sort_blocks(columns)
    u_rows = jnp.swapaxes(u_factor, 3, 4).reshape(320, 32, 256)
    v_rows = jnp.swapaxes(v_factor, 3, 4).reshape(320, 32, 256)
    grams, rows = sum_sketches(slots, places, ranks.reshape(320), omega[0], u_rows, v_rows)
    return factor(grams, rows)


def solution(mesh):
    placed = (
        P("grp", "dev", None, None),
        P("grp", "dev", None, None, None),
        P("grp", "dev", None, None, None),
        P("grp", "dev", None, None),
        P("grp", "dev", None),
    )
    return jax.shard_map(
        on_device,
        mesh=mesh,
        in_specs=placed,
        out_specs=(P("dev", "grp", None), P("dev", None, None)),
        check_vma=False,
    )
```

```python
import functools
import jax
import jax.numpy as jnp
from jax import lax
from jax.experimental import pallas as pl
from jax.experimental.pallas import tpu as pltpu
from jax.sharding import PartitionSpec as P

precise = lax.Precision.HIGHEST


GROUP = 5
SEGS = ((0, 4), (4, 8), (8, 12), (12, 16))

def pick_lane(x, lane):
    idx = jnp.full(x.shape, lane, jnp.int32)
    return jnp.take_along_axis(x, idx, axis=1)

def factor_all(work, mats, spans=SEGS):
    sub = lax.broadcasted_iota(jnp.int32, (8, 128), 0)
    lane = lax.broadcasted_iota(jnp.int32, (8, 128), 1)

    def split(x):
        h = x.astype(jnp.bfloat16).astype(jnp.float32)
        rest = x - h
        d = rest.astype(jnp.bfloat16).astype(jnp.float32)
        return h, d, rest - d

    def panel(k, top):
        base = pl.multiple_of(k * 8, 8)
        raw = [work[m, pl.ds(base, 8), :] for m in mats]
        keep = lane >= base + sub
        below = lane >= base + 8
        prods = []
        rows = []
        for g in range(0, len(mats), GROUP):
            part = raw[g:g + GROUP]
            ps = [x[:, 0:128] for x in part]
            qs = [x[:, 128:256] for x in part]
            cols = [[pick_lane(p, base + r) for r in range(8)] for p in ps]
            for r in range(8):
                for i in range(len(part)):
                    c = cols[i][r]
                    inv = lax.rsqrt(jnp.broadcast_to(c[r:r + 1], (8, 128)))
                    cs = c * inv
                    prow = ps[i][r:r + 1] * inv
                    qrow = qs[i][r:r + 1] * inv
                    cz = jnp.where(sub > r, cs, 0.0)
                    ps[i] = jnp.where(sub == r, prow, ps[i] - cz * prow)
                    qs[i] = jnp.where(sub == r, qrow, qs[i] - cz * qrow)
                    for t in range(r + 1, 8):
                        cols[i][t] = cols[i][t] - cs * cs[t:t + 1]
            for i in range(len(part)):
                p = jnp.where(keep, ps[i], 0.0)
                full = jnp.concatenate([p, qs[i]], axis=1)
                rows.append(full)
                ph, pd, pe = split(jnp.where(below, p, 0.0))
                fh, fd, fe = split(full)
                left = jnp.concatenate([ph, ph, pd, ph, pe, pd], axis=0)
                right = jnp.concatenate([fh, fd, fh, fe, fh, fd], axis=0)
                leftT = left.T[top:].astype(jnp.bfloat16)
                prods.append(lax.dot_general(leftT, right.astype(jnp.bfloat16), (((1,), (0,)), ((), ())), preferred_element_type=jnp.float32))
        for m, full, prod in zip(mats, rows, prods):
            work[m, pl.ds(base, 8), :] = full
        for m, full, prod in zip(mats, rows, prods):
            work[m, top:128, :] = work[m, top:128, :] - prod

    for lo, hi in spans:
        def body(k, _, lo=lo):
            panel(k, lo * 8)
            return 0
        lax.fori_loop(lo, hi, body, 0)


def init_work(work, m, gram):
    r = lax.broadcasted_iota(jnp.int32, (128, 128), 0)
    c = lax.broadcasted_iota(jnp.int32, (128, 128), 1)
    work[m, :, 0:128] = gram
    work[m, :, 128:256] = jnp.where(r == c, 1.0, 0.0)


NODES = ((0, 1, 4), (2, 3, 5), (4, 5, 6), (7, 8, 9))


def times_transposed(x, y):
    return lax.dot_general(x, y, (((1,), (1,)), ((), ())), precision=precise, preferred_element_type=jnp.float32)


def write_node(work, n, transfer_ref):
    left, right, parent = NODES[n]
    inverse = work[parent, :, 128:256]
    for half, child in enumerate((left, right)):
        made = times_transposed(work[child, :, 0:128], inverse)
        if n == 3:
            made = jnp.where(lax.axis_index("dev") == lax.axis_size("dev") - 1, 0.0, made)
        transfer_ref[n, half * 128 : (half + 1) * 128, :] = made


RIGHT, LEFT, DOWN, UP, ACROSS = range(5)


def split_two(x):
    high = x.astype(jnp.bfloat16)
    low = (x - high.astype(jnp.float32)).astype(jnp.bfloat16)
    return high, low


def bf16_dot(x, y):
    return lax.dot_general(x, y, (((1,), (0,)), ((), ())), preferred_element_type=jnp.float32)


def sort_blocks(column_ref, named, places, slots):
    lane = lax.broadcasted_iota(jnp.int32, (128, 128), 1)
    down = lax.broadcasted_iota(jnp.int32, (128, 128), 0)
    named[...] = jnp.full((8, 128), -1, jnp.int32)
    for i in range(4):
        named[i : i + 1, 0:80] = column_ref[i]
    rows = named[...]
    turned = rows.T
    places[...] = jnp.full((8, 128), -1, jnp.int32)
    for i in range(4):
        row = jnp.broadcast_to(rows[i : i + 1], (128, 128))
        turn = ((turned[:, i : i + 1] == row) & (down < lane)).astype(jnp.int32)
        for other in range(i):
            turn = turn + (turned[:, other : other + 1] == row).astype(jnp.int32)
        place = jnp.minimum(jnp.sum(turn, axis=0, keepdims=True), 2) * 128 + rows[i : i + 1]
        places[i : i + 1] = jnp.where(lane[0:1] < 80, place, -1)
    turned = places[...].T
    slots[...] = jnp.zeros((8, 128), jnp.int32)
    for t in range(3):
        block = jnp.zeros((128, 128), jnp.int32)
        for i in range(4):
            block = block + jnp.where(turned[:, i : i + 1] == lane + t * 128, down + i * 80, 0)
        slots[t : t + 1] = jnp.minimum(jnp.sum(block, axis=0, keepdims=True), 319)


def sum_kernel(
    column_ref, rank_ref, omega_ref, u_ref, v_ref, state_ref, rows_ref, child_ref,
    probe, u_all, v_all, u_high, u_low, coeff, weights,
    sketch, relay, parts, whole, leaf_gram, leaf_rows, top_gram, tree, eights, work, children,
    named, places, slots, place_at, slot_at,
    load_sem, send_sem, recv_sem, out_sem, in_sem,
):
    me = lax.axis_index("dev")
    core = me % 2
    x_at = me // 2 % 4
    y_at = me // 8
    partner = me + 1 - 2 * core

    def device(dy, dx):
        return ((y_at + dy) % 4 * 4 + (x_at + dx) % 4) * 2 + core

    targets = (device(0, 1), device(0, 3), device(1, 0), device(3, 0), partner)
    own = pltpu.make_async_copy(omega_ref, probe.at[pl.ds(me * 4, 4)], load_sem.at[0])
    own.start()
    loads = [
        pltpu.make_async_copy(v_ref, v_all, load_sem.at[1]),
        pltpu.make_async_copy(u_ref, u_all, load_sem.at[2]),
    ]
    for load in loads:
        load.start()
    z = lax.axis_index("grp")
    e = me % 8
    barrier = pltpu.get_barrier_semaphore()
    peers = [{"dev": me // 8 * 8 + (e + n) % 8} for n in range(1, 8)]
    peers += [{"dev": (me + 8 * n) % 32} for n in range(1, 4)]
    peers += [{"grp": (z + n) % 4} for n in range(1, 4)]
    for peer in peers:
        pl.semaphore_signal(barrier, inc=1, device_id=peer, device_id_type=pl.DeviceIdType.MESH)
    sort_blocks(column_ref, named, places, slots)
    tables = [
        pltpu.make_async_copy(places, place_at, load_sem.at[3]),
        pltpu.make_async_copy(slots, slot_at, load_sem.at[4]),
    ]
    pl.semaphore_wait(barrier, 13)
    own.wait()
    for table in tables:
        table.start()

    def move(cluster, way):
        return pltpu.make_async_remote_copy(
            src_ref=probe.at[cluster],
            dst_ref=probe.at[cluster],
            send_sem=send_sem.at[way],
            recv_sem=recv_sem.at[cluster],
            device_id={"dev": targets[way]},
            device_id_type=pl.DeviceIdType.MESH,
        )

    def await_cluster(cluster):
        move(cluster, RIGHT).wait_recv()

    def make_coeff(cluster):
        wide = jnp.concatenate(split_two(probe[cluster]), axis=1)
        rows = jnp.concatenate([v_all[slot_at[t, cluster]] for t in range(3)], axis=0)
        high, low = split_two(rows)
        both = bf16_dot(high, wide)
        made = both[:, 0:128] + both[:, 128:256] + bf16_dot(low, wide[:, 0:128])
        packed = jnp.concatenate(split_two(made), axis=1)
        for t in range(3):
            coeff[t * 128 + cluster] = packed[t * 32 : t * 32 + 32]

    rank_row = lax.broadcasted_iota(jnp.int32, (32, 256), 0)

    def turn_rows(chunk):
        pieces = [
            jnp.where(rank_row < rank_ref[chunk // 10, chunk % 10 * 8 + e], u_all[chunk * 8 + e], 0.0) for e in range(8)
        ]
        high, low = split_two(jnp.concatenate(pieces, axis=0).T)
        leaf = chunk // 10
        where = pl.ds(pl.multiple_of(chunk % 10 * 256, 256), 256)
        u_high[leaf, :, where] = high
        u_low[leaf, :, where] = low

    def step(dy, dx, j, before, first=False, chunk=None):
        along_x = device(dy, dx) * 4 + j
        along_y = device(dx, dy) * 4 + j + 2
        flips = ((along_x, (RIGHT, LEFT, DOWN, UP)), (along_y, (DOWN, UP, RIGHT, LEFT)))
        for cluster, (ahead, back, out, home) in flips:
            if not first:
                await_cluster(cluster)
            ways = []
            if isinstance(dy, int) and dy == 0:
                if first:
                    ways += [ahead, back]
                elif dx == 3 and j == 0:
                    ways += [ahead]
                elif dx == 1 and j == 1:
                    ways += [back]
                ways += [out, home]
            elif dy == 3 and j == 0:
                ways += [out]
            elif dy == 1 and j == 1:
                ways += [home]
            for way in ways + [ACROSS]:
                move(cluster, way).start()
        now = [along_x, along_y]
        work = list(now)
        if before is not None:
            for cluster in before:
                await_cluster(cluster)
                work.append(cluster)
        if first and j == 0:
            loads[0].wait()
            for table in tables:
                table.wait()
        for cluster in work:
            make_coeff(cluster)
        if chunk is not None:
            turn_rows(chunk)
            turn_rows(chunk + 1)
        shift = 4 - 8 * core
        return [c + shift for c in now]

    late = step(0, 0, 0, None, first=True)
    late = step(0, 0, 1, late, first=True)
    loads[1].wait()

    def turn_some(chunk, carry):
        turn_rows(chunk)
        return carry

    lax.fori_loop(0, 8, turn_some, 0)
    for dx, j in ((3, 0), (1, 1), (3, 1), (1, 0), (2, 0), (2, 1)):
        late = step(0, dx, j, late)

    def far(q):
        return jnp.where(q == 0, 0, jnp.where(q == 1, 3, q - 1))

    def cross(q, late):
        for s, (dy, j) in enumerate(((3, 0), (1, 1), (3, 1), (1, 0))):
            late = step(dy, far(q), j, late, chunk=8 + q * 8 + s * 2)
        return tuple(late)

    def end(q, late):
        for j in range(2):
            late = step(2, far(q), j, late)
        return tuple(late)

    late = lax.fori_loop(0, 4, cross, tuple(late))
    late = lax.fori_loop(0, 4, end, late)
    for cluster in late:
        await_cluster(cluster)
    for cluster in late:
        make_coeff(cluster)

    def sketch_leaf(leaf):
        for b in range(80):
            weights[b * 32 : b * 32 + 32, :] = coeff[place_at[leaf, b]]
        both = bf16_dot(u_high[leaf], weights[...])
        sketch[leaf] = both[:, 0:128] + both[:, 128:256] + bf16_dot(u_low[leaf], weights[:, 0:128])

    def send(source, target, out, arrival, peer):
        return pltpu.make_async_remote_copy(
            src_ref=source,
            dst_ref=target,
            send_sem=out_sem.at[out],
            recv_sem=in_sem.at[arrival],
            device_id=peer,
            device_id_type=pl.DeviceIdType.MESH,
        )

    top, bottom = pl.ds(0, 128), pl.ds(128, 128)
    after, across_z, before = [(z + n) % 4 for n in (1, 2, 3)]
    to_after, to_across, to_before = [{"grp": n} for n in (after, across_z, before)]
    far_out = send(sketch.at[across_z, top], relay.at[0], 0, 0, to_after)
    far_home = send(sketch.at[across_z, bottom], relay.at[1], 1, 1, to_before)
    near_out = send(sketch.at[after, bottom], parts.at[0], 2, 2, to_after)
    near_home = send(sketch.at[before, top], parts.at[1], 3, 3, to_before)
    joint_out = send(sketch.at[after, top], parts.at[2], 4, 4, to_after)
    joint_home = send(sketch.at[before, bottom], parts.at[3], 5, 5, to_before)

    def leaf_step(n, carry):
        sketch_leaf((z + jnp.where(n == 0, 2, jnp.where(n == 1, 1, jnp.where(n == 2, 3, 0)))) % 4)

        @pl.when(n == 0)
        def _():
            far_out.start()
            far_home.start()

        @pl.when(n == 1)
        def _():
            near_out.start()

        @pl.when(n == 2)
        def _():
            near_home.start()

        return carry

    lax.fori_loop(0, 4, leaf_step, 0)
    far_out.wait_recv()
    sketch[after, 0:128] = sketch[after, 0:128] + relay[0]
    joint_out.start()
    far_home.wait_recv()
    sketch[before, 128:256] = sketch[before, 128:256] + relay[1]
    joint_home.start()
    near_out.wait_recv()
    near_home.wait_recv()
    joint_out.wait_recv()
    whole[0:128] = sketch[z, 0:128] + parts[1] + parts[2]
    joint_home.wait_recv()
    whole[128:256] = sketch[z, 128:256] + parts[0] + parts[3]
    flat = whole[...]
    leaf_gram[z] = lax.dot_general(
        flat.T, flat, (((1,), (0,)), ((), ())), precision=precise, preferred_element_type=jnp.float32
    )
    others = ((2, across_z, to_across), (1, after, to_after), (3, before, to_before))
    gram_sends = [send(leaf_gram.at[z], leaf_gram.at[z], 5 + n, 6 + z, peer) for n, _, peer in others]
    row_sends = [
        send(whole.at[pl.ds(pl.multiple_of(there * 64, 64), 64)], leaf_rows.at[z], 8 + n, 10 + z, peer)
        for n, there, peer in others
    ]
    for copy in gram_sends:
        copy.start()
    leaf_rows[z] = whole[pl.ds(pl.multiple_of(z * 64, 64), 64)]
    for _, there, peer in others:
        send(leaf_gram.at[there], leaf_gram.at[there], 6, 6 + there, peer).wait_recv()
    first_pair = leaf_gram[0] + leaf_gram[1]
    second_pair = leaf_gram[2] + leaf_gram[3]
    own_top = first_pair + second_pair
    top_gram[...] = own_top

    def tree_send(slot, target):
        return send(top_gram, tree.at[e], 12 + slot, 14 + e, {"dev": me // 8 * 8 + target})

    tree_sends = (
        (e != 7, tree_send(0, 7)),
        (e != 3, tree_send(1, 3)),
        (e % 4 != 1, tree_send(2, e // 4 * 4 + 1)),
        (e % 2 == 1, tree_send(3, e - 1)),
    )
    for needed, copy in tree_sends:
        pl.when(needed)(copy.start)
    for copy in row_sends:
        copy.start()
    for m, gram in enumerate([leaf_gram[c] for c in range(4)] + [first_pair, second_pair, own_top]):
        init_work(work, m, gram)
    factor_all(work, range(7), SEGS[:2])

    def arrived(slot):
        send(top_gram, tree.at[slot], 12, 14 + slot, to_after).wait_recv()
        return tree[slot]

    def keep(left, right):
        children[0] = left
        children[1] = right

    def eight_send(slot, row):
        return send(top_gram, eights.at[y_at], 16 + slot, 22 + y_at, {"dev": row * 8 + 7})

    eight_sends = (
        (e * 4 + y_at == 28, eight_send(0, 1)),
        (e * 4 + y_at == 29, eight_send(0, 0)),
        (e * 4 + y_at == 30, eight_send(0, 1)),
        (e * 4 + y_at == 31, eight_send(0, 1)),
        (e * 4 + y_at == 31, eight_send(1, 2)),
    )

    @pl.when(e == 7)
    def _():
        pairs = [arrived(0) + arrived(1), arrived(2) + arrived(3), arrived(4) + arrived(5), arrived(6) + own_top]
        for needed, copy in tree_sends:
            pl.when(needed)(copy.wait_send)
        eight = (pairs[0] + pairs[1]) + (pairs[2] + pairs[3])
        top_gram[...] = eight
        for needed, copy in eight_sends:
            pl.when(needed)(copy.start)

    factor_all(work, range(7), SEGS[2:])
    for _, there, peer in others:
        send(leaf_rows.at[there], leaf_rows.at[there], 9, 10 + there, peer).wait_recv()
    results = [
        pltpu.make_async_copy(work.at[pl.ds(0, 7)], state_ref, load_sem.at[0]),
        pltpu.make_async_copy(leaf_rows, rows_ref, load_sem.at[1]),
        pltpu.make_async_copy(children, child_ref, load_sem.at[2]),
    ]
    results[0].start()
    results[1].start()

    @pl.when(e % 2 == 0)
    def _():
        keep(own_top, arrived(e + 1))

    @pl.when(e % 4 == 1)
    def _():
        keep(arrived(e - 1) + own_top, arrived(e + 1) + arrived(e + 2))

    @pl.when(e == 3)
    def _():
        left = arrived(0) + arrived(1) + (arrived(2) + own_top)
        keep(left, arrived(4) + arrived(5) + (arrived(6) + arrived(7)))

    @pl.when(e == 7)
    def _():
        eight = top_gram[...]

        def landed(row):
            send(top_gram, eights.at[row], 16, 22 + row, to_after).wait_recv()
            return eights[row]

        @pl.when(y_at == 0)
        def _():
            keep(eight, landed(1))

        @pl.when(y_at == 1)
        def _():
            keep(landed(0) + eight, landed(2) + landed(3))

        @pl.when(y_at == 2)
        def _():
            keep(eight, landed(3))

        @pl.when(y_at == 3)
        def _():
            keep(eight, eight)

        for needed, copy in eight_sends:
            pl.when(needed)(copy.wait_send)

    @pl.when(e != 7)
    def _():
        for needed, copy in tree_sends:
            pl.when(needed)(copy.wait_send)

    results[2].start()
    for copy in [far_out, far_home, near_out, near_home, joint_out, joint_home] + gram_sends + row_sends:
        copy.wait_send()
    for way in range(4):
        span = pl.ds(0, 15)
        pltpu.make_async_remote_copy(
            src_ref=probe.at[span], dst_ref=probe.at[span], send_sem=send_sem.at[way], recv_sem=recv_sem.at[0],
            device_id={"dev": targets[way]}, device_id_type=pl.DeviceIdType.MESH,
        ).wait_send()
    span = pl.ds(0, 64)
    pltpu.make_async_remote_copy(
        src_ref=probe.at[span], dst_ref=probe.at[span], send_sem=send_sem.at[ACROSS], recv_sem=recv_sem.at[0],
        device_id={"dev": partner}, device_id_type=pl.DeviceIdType.MESH,
    ).wait_send()
    for result in results:
        result.wait()


def sum_and_factor(columns, ranks, omega, u_rows, v_rows):
    smem = pl.BlockSpec(memory_space=pltpu.SMEM)
    anywhere = pl.BlockSpec(memory_space=pl.ANY)
    return pl.pallas_call(
        sum_kernel,
        out_shape=(
            jax.ShapeDtypeStruct((7, 128, 256), jnp.float32),
            jax.ShapeDtypeStruct((4, 64, 128), jnp.float32),
            jax.ShapeDtypeStruct((2, 128, 128), jnp.float32),
        ),
        in_specs=[pl.BlockSpec(memory_space=pltpu.VMEM), smem, anywhere, anywhere, anywhere],
        out_specs=(anywhere, anywhere, anywhere),
        scratch_shapes=[
            pltpu.VMEM((128, 256, 128), jnp.float32),
            pltpu.VMEM((320, 32, 256), jnp.float32),
            pltpu.VMEM((320, 32, 256), jnp.float32),
            pltpu.VMEM((4, 256, 2560), jnp.bfloat16),
            pltpu.VMEM((4, 256, 2560), jnp.bfloat16),
            pltpu.VMEM((384, 32, 256), jnp.bfloat16),
            pltpu.VMEM((2560, 256), jnp.bfloat16),
            pltpu.VMEM((4, 256, 128), jnp.float32),
            pltpu.VMEM((2, 128, 128), jnp.float32),
            pltpu.VMEM((4, 128, 128), jnp.float32),
            pltpu.VMEM((256, 128), jnp.float32),
            pltpu.VMEM((4, 128, 128), jnp.float32),
            pltpu.VMEM((4, 64, 128), jnp.float32),
            pltpu.VMEM((128, 128), jnp.float32),
            pltpu.VMEM((8, 128, 128), jnp.float32),
            pltpu.VMEM((4, 128, 128), jnp.float32),
            pltpu.VMEM((7, 128, 256), jnp.float32),
            pltpu.VMEM((2, 128, 128), jnp.float32),
            pltpu.VMEM((8, 128), jnp.int32),
            pltpu.VMEM((8, 128), jnp.int32),
            pltpu.VMEM((8, 128), jnp.int32),
            pltpu.SMEM((8, 128), jnp.int32),
            pltpu.SMEM((8, 128), jnp.int32),
            pltpu.SemaphoreType.DMA((5,)),
            pltpu.SemaphoreType.DMA((5,)),
            pltpu.SemaphoreType.DMA((128,)),
            pltpu.SemaphoreType.DMA((18,)),
            pltpu.SemaphoreType.DMA((26,)),
        ],
        compiler_params=pltpu.CompilerParams(
            collective_id=0, has_side_effects=True, vmem_limit_bytes=62 * 2**20
        ),
        name="recompress",
    )(columns, ranks, omega, u_rows, v_rows)


def finish_kernel(child_ref, state_ref, rows_ref, basis_ref, transfer_ref, work, rows, basis, transfer, sem):
    loads = [
        pltpu.make_async_copy(state_ref, work.at[pl.ds(0, 7)], sem.at[0]),
        pltpu.make_async_copy(rows_ref, rows, sem.at[1]),
    ]
    for load in loads:
        load.start()
    init_work(work, 7, child_ref[0])
    init_work(work, 8, child_ref[1])
    init_work(work, 9, child_ref[0] + child_ref[1])
    factor_all(work, range(7, 10), SEGS[:1])
    for load in loads:
        load.wait()
    for c in range(4):
        basis[c] = times_transposed(rows[c], work[c, :, 128:256])
    for n in range(3):
        write_node(work, n, transfer)
    early, late = pl.ds(0, 3), pl.ds(3, 1)
    stores = [
        pltpu.make_async_copy(basis, basis_ref, sem.at[2]),
        pltpu.make_async_copy(transfer.at[early], transfer_ref.at[early], sem.at[3]),
        pltpu.make_async_copy(transfer.at[late], transfer_ref.at[late], sem.at[4]),
    ]
    stores[0].start()
    stores[1].start()
    factor_all(work, range(7, 10), SEGS[1:])
    write_node(work, 3, transfer)
    stores[2].start()
    for store in stores:
        store.wait()


def finish(state, rows, children):
    vmem = pl.BlockSpec(memory_space=pltpu.VMEM)
    anywhere = pl.BlockSpec(memory_space=pl.ANY)
    return pl.pallas_call(
        finish_kernel,
        out_shape=(
            jax.ShapeDtypeStruct((4, 64, 128), jnp.float32),
            jax.ShapeDtypeStruct((4, 256, 128), jnp.float32),
        ),
        in_specs=[vmem, anywhere, anywhere],
        out_specs=(anywhere, anywhere),
        scratch_shapes=[
            pltpu.VMEM((10, 128, 256), jnp.float32),
            pltpu.VMEM((4, 64, 128), jnp.float32),
            pltpu.VMEM((4, 64, 128), jnp.float32),
            pltpu.VMEM((4, 256, 128), jnp.float32),
            pltpu.SemaphoreType.DMA((5,)),
        ],
        compiler_params=pltpu.CompilerParams(vmem_limit_bytes=62 * 2**20),
        name="finish",
    )(children, state, rows)


def on_device(omega, u_factor, v_factor, columns, ranks):
    u_rows = jnp.swapaxes(u_factor, 3, 4).reshape(320, 32, 256)
    v_rows = jnp.swapaxes(v_factor, 3, 4).reshape(320, 32, 256)
    named = jnp.swapaxes(columns[0], 1, 2)
    state, rows, children = sum_and_factor(named, ranks[0], omega[0], u_rows, v_rows)
    return finish(state, rows, children)


def solution(mesh):
    placed = (
        P("grp", "dev", None, None),
        P("grp", "dev", None, None, None),
        P("grp", "dev", None, None, None),
        P("grp", "dev", None, None),
        P("grp", "dev", None),
    )
    return jax.shard_map(
        on_device,
        mesh=mesh,
        in_specs=placed,
        out_specs=(P("dev", "grp", None), P("dev", None, None)),
        check_vma=False,
    )
```

```python
import functools
import jax
import jax.numpy as jnp
from jax import lax
from jax.experimental import pallas as pl
from jax.experimental.pallas import tpu as pltpu
from jax.sharding import PartitionSpec as P

precise = lax.Precision.HIGHEST


SEGS = ((0, 2), (2, 4), (4, 6), (6, 8))


def pick_lane(x, lane):
    idx = jnp.full(x.shape, lane, jnp.int32)
    return jnp.take_along_axis(x, idx, axis=1)


def make_panel(work, mats, group):
    sub = lax.broadcasted_iota(jnp.int32, (8, 128), 0)
    lane = lax.broadcasted_iota(jnp.int32, (8, 128), 1)

    def split(x):
        h = x.astype(jnp.bfloat16).astype(jnp.float32)
        rest = x - h
        d = rest.astype(jnp.bfloat16).astype(jnp.float32)
        return h, d, rest - d

    def panel(k, top):
        base = k * 16 if isinstance(k, int) else pl.multiple_of(k * 16, 16)
        raw = [work[m, pl.ds(base, 16), :] for m in mats]
        prods = []
        rows = []
        for g in range(0, len(mats), group):
            part = raw[g : g + group]
            ps = [[x[0:8, 0:128], x[8:16, 0:128]] for x in part]
            qs = [[x[0:8, 128:256], x[8:16, 128:256]] for x in part]
            high = [[pick_lane(p[0], base + r) for r in range(8)] for p in ps]
            low = [[pick_lane(p[1], base + r) for r in range(16)] for p in ps]
            for r in range(16):
                h, n = r // 8, r % 8
                for p, q, up, down in zip(ps, qs, high, low):
                    pivot = (up if h == 0 else down)[r][n : n + 1]
                    inv = lax.rsqrt(jnp.broadcast_to(pivot, (8, 128)))
                    prow = p[h][n : n + 1] * inv
                    qrow = q[h][n : n + 1] * inv
                    below = down[r] * inv
                    if h == 0:
                        here = up[r] * inv
                        p[1] = p[1] - below * prow
                        q[1] = q[1] - below * qrow
                        for t in range(r + 1, 8):
                            up[t] = up[t] - here * here[t : t + 1]
                            down[t] = down[t] - below * here[t : t + 1]
                    else:
                        here = below
                    for t in range(max(r + 1, 8), 16):
                        down[t] = down[t] - below * below[t - 8 : t - 7]
                    rest = jnp.where(sub > n, here, 0.0)
                    p[h] = jnp.where(sub == n, prow, p[h] - rest * prow)
                    q[h] = jnp.where(sub == n, qrow, q[h] - rest * qrow)
            for p, q in zip(ps, qs):
                both = [jnp.where(lane >= base + 8 * h + sub, p[h], 0.0) for h in range(2)]
                full = jnp.concatenate([jnp.concatenate(both, axis=0), jnp.concatenate(q, axis=0)], axis=1)
                rows.append(full)
                if top == 128:
                    continue
                after = [jnp.where(lane >= base + 16, x, 0.0) for x in both]
                ph, pd, pe = split(jnp.concatenate(after, axis=0))
                fh, fd, fe = split(full)
                left = jnp.concatenate([ph, ph, pd, ph, pe, pd], axis=0)
                right = jnp.concatenate([fh, fd, fh, fe, fh, fd], axis=0)
                turned = left.T[top:].astype(jnp.bfloat16)
                prods.append(
                    lax.dot_general(
                        turned,
                        right.astype(jnp.bfloat16),
                        (((1,), (0,)), ((), ())),
                        preferred_element_type=jnp.float32,
                    )
                )
        for m, full in zip(mats, rows):
            work[m, pl.ds(base, 16), :] = full
        for m, prod in zip(mats, prods):
            work[m, top:128, :] = work[m, top:128, :] - prod

    return panel


def factor_span(work, mats, spans):
    panel = make_panel(work, mats, 4)
    for lo, hi in spans:
        def body(k, _, lo=lo):
            panel(k, lo * 16)
            return 0
        lax.fori_loop(lo, hi, body, 0)


def init_work(work, m, gram):
    r = lax.broadcasted_iota(jnp.int32, (128, 128), 0)
    c = lax.broadcasted_iota(jnp.int32, (128, 128), 1)
    work[m, :, 0:128] = gram
    work[m, :, 128:256] = jnp.where(r == c, 1.0, 0.0)


NODES = ((0, 1, 4), (2, 3, 5), (4, 5, 6), (7, 8, 9))


def times_transposed(x, y):
    return lax.dot_general(x, y, (((1,), (1,)), ((), ())), precision=precise, preferred_element_type=jnp.float32)


def write_node(work, n, transfer_ref):
    left, right, parent = NODES[n]
    inverse = work[parent, :, 128:256]
    for half, child in enumerate((left, right)):
        made = times_transposed(work[child, :, 0:128], inverse)
        if n == 3:
            made = jnp.where(lax.axis_index("dev") == lax.axis_size("dev") - 1, 0.0, made)
        transfer_ref[n, half * 128 : (half + 1) * 128, :] = made


RIGHT, LEFT, DOWN, UP, ACROSS = range(5)


def split_two(x):
    high = x.astype(jnp.bfloat16)
    low = (x - high.astype(jnp.float32)).astype(jnp.bfloat16)
    return high, low


def bf16_dot(x, y):
    return lax.dot_general(x, y, (((1,), (0,)), ((), ())), preferred_element_type=jnp.float32)


def sort_blocks(column_ref, named, places, slots):
    lane = lax.broadcasted_iota(jnp.int32, (128, 128), 1)
    down = lax.broadcasted_iota(jnp.int32, (128, 128), 0)
    named[...] = jnp.full((8, 128), -1, jnp.int32)
    for i in range(4):
        named[i : i + 1, 0:80] = column_ref[i]
    rows = named[...]
    turned = rows.T
    places[...] = jnp.full((8, 128), -1, jnp.int32)
    for i in range(4):
        row = jnp.broadcast_to(rows[i : i + 1], (128, 128))
        turn = ((turned[:, i : i + 1] == row) & (down < lane)).astype(jnp.int32)
        for other in range(i):
            turn = turn + (turned[:, other : other + 1] == row).astype(jnp.int32)
        place = jnp.minimum(jnp.sum(turn, axis=0, keepdims=True), 2) * 128 + rows[i : i + 1]
        places[i : i + 1] = jnp.where(lane[0:1] < 80, place, -1)
    turned = places[...].T
    slots[...] = jnp.zeros((8, 128), jnp.int32)
    for t in range(3):
        block = jnp.zeros((128, 128), jnp.int32)
        for i in range(4):
            block = block + jnp.where(turned[:, i : i + 1] == lane + t * 128, down + i * 80, 0)
        slots[t : t + 1] = jnp.minimum(jnp.sum(block, axis=0, keepdims=True), 319)


def sum_kernel(
    column_ref, rank_ref, omega_ref, u_ref, v_ref, state_ref, rows_ref, child_ref,
    probe, u_all, v_all, u_high, u_low, coeff, weights,
    sketch, relay, parts, whole, leaf_gram, leaf_rows, top_gram, tree, eights, work, children,
    named, places, slots, place_at, slot_at,
    load_sem, send_sem, recv_sem, out_sem, in_sem,
):
    me = lax.axis_index("dev")
    core = me % 2
    x_at = me // 2 % 4
    y_at = me // 8
    partner = me + 1 - 2 * core

    def device(dy, dx):
        return ((y_at + dy) % 4 * 4 + (x_at + dx) % 4) * 2 + core

    targets = (device(0, 1), device(0, 3), device(1, 0), device(3, 0), partner)
    own = pltpu.make_async_copy(omega_ref, probe.at[pl.ds(me * 4, 4)], load_sem.at[0])
    own.start()
    loads = [
        pltpu.make_async_copy(v_ref, v_all, load_sem.at[1]),
        pltpu.make_async_copy(u_ref, u_all, load_sem.at[2]),
    ]
    for load in loads:
        load.start()
    z = lax.axis_index("grp")
    e = me % 8
    barrier = pltpu.get_barrier_semaphore()
    peers = [{"dev": me // 8 * 8 + (e + n) % 8} for n in range(1, 8)]
    peers += [{"dev": (me + 8 * n) % 32} for n in range(1, 4)]
    peers += [{"grp": (z + n) % 4} for n in range(1, 4)]
    for peer in peers:
        pl.semaphore_signal(barrier, inc=1, device_id=peer, device_id_type=pl.DeviceIdType.MESH)
    sort_blocks(column_ref, named, places, slots)
    tables = [
        pltpu.make_async_copy(places, place_at, load_sem.at[3]),
        pltpu.make_async_copy(slots, slot_at, load_sem.at[4]),
    ]
    pl.semaphore_wait(barrier, 13)
    own.wait()
    for table in tables:
        table.start()

    def move(cluster, way):
        return pltpu.make_async_remote_copy(
            src_ref=probe.at[cluster],
            dst_ref=probe.at[cluster],
            send_sem=send_sem.at[way],
            recv_sem=recv_sem.at[cluster],
            device_id={"dev": targets[way]},
            device_id_type=pl.DeviceIdType.MESH,
        )

    def await_cluster(cluster):
        move(cluster, RIGHT).wait_recv()

    def make_coeff(cluster):
        wide = jnp.concatenate(split_two(probe[cluster]), axis=1)
        rows = jnp.concatenate([v_all[slot_at[t, cluster]] for t in range(3)], axis=0)
        high, low = split_two(rows)
        both = bf16_dot(high, wide)
        made = both[:, 0:128] + both[:, 128:256] + bf16_dot(low, wide[:, 0:128])
        packed = jnp.concatenate(split_two(made), axis=1)
        for t in range(3):
            coeff[t * 128 + cluster] = packed[t * 32 : t * 32 + 32]

    rank_row = lax.broadcasted_iota(jnp.int32, (32, 256), 0)

    def turn_rows(chunk):
        pieces = [
            jnp.where(rank_row < rank_ref[chunk // 10, chunk % 10 * 8 + e], u_all[chunk * 8 + e], 0.0) for e in range(8)
        ]
        high, low = split_two(jnp.concatenate(pieces, axis=0).T)
        leaf = chunk // 10
        where = pl.ds(pl.multiple_of(chunk % 10 * 256, 256), 256)
        u_high[leaf, :, where] = high
        u_low[leaf, :, where] = low

    def step(dy, dx, j, before, first=False, chunk=None):
        along_x = device(dy, dx) * 4 + j
        along_y = device(dx, dy) * 4 + j + 2
        flips = ((along_x, (RIGHT, LEFT, DOWN, UP)), (along_y, (DOWN, UP, RIGHT, LEFT)))
        for cluster, (ahead, back, out, home) in flips:
            if not first:
                await_cluster(cluster)
            ways = []
            if isinstance(dy, int) and dy == 0:
                if first:
                    ways += [ahead, back]
                elif dx == 3 and j == 0:
                    ways += [ahead]
                elif dx == 1 and j == 1:
                    ways += [back]
                ways += [out, home]
            elif dy == 3 and j == 0:
                ways += [out]
            elif dy == 1 and j == 1:
                ways += [home]
            for way in ways + [ACROSS]:
                move(cluster, way).start()
        now = [along_x, along_y]
        work = list(now)
        if before is not None:
            for cluster in before:
                await_cluster(cluster)
                work.append(cluster)
        if first and j == 0:
            loads[0].wait()
            for table in tables:
                table.wait()
        for cluster in work:
            make_coeff(cluster)
        if chunk is not None:
            turn_rows(chunk)
            turn_rows(chunk + 1)
        shift = 4 - 8 * core
        return [c + shift for c in now]

    late = step(0, 0, 0, None, first=True)
    late = step(0, 0, 1, late, first=True)
    loads[1].wait()

    def turn_some(chunk, carry):
        turn_rows(chunk)
        return carry

    lax.fori_loop(0, 8, turn_some, 0)
    for dx, j in ((3, 0), (1, 1), (3, 1), (1, 0), (2, 0), (2, 1)):
        late = step(0, dx, j, late)

    def far(q):
        return jnp.where(q == 0, 0, jnp.where(q == 1, 3, q - 1))

    def cross(q, late):
        for s, (dy, j) in enumerate(((3, 0), (1, 1), (3, 1), (1, 0))):
            late = step(dy, far(q), j, late, chunk=8 + q * 8 + s * 2)
        return tuple(late)

    def end(q, late):
        for j in range(2):
            late = step(2, far(q), j, late)
        return tuple(late)

    late = lax.fori_loop(0, 4, cross, tuple(late))
    late = lax.fori_loop(0, 4, end, late)
    for cluster in late:
        await_cluster(cluster)
    for cluster in late:
        make_coeff(cluster)

    def sketch_leaf(leaf):
        for b in range(80):
            weights[b * 32 : b * 32 + 32, :] = coeff[place_at[leaf, b]]
        both = bf16_dot(u_high[leaf], weights[...])
        sketch[leaf] = both[:, 0:128] + both[:, 128:256] + bf16_dot(u_low[leaf], weights[:, 0:128])

    def send(source, target, out, arrival, peer):
        return pltpu.make_async_remote_copy(
            src_ref=source,
            dst_ref=target,
            send_sem=out_sem.at[out],
            recv_sem=in_sem.at[arrival],
            device_id=peer,
            device_id_type=pl.DeviceIdType.MESH,
        )

    top, bottom = pl.ds(0, 128), pl.ds(128, 128)
    after, across_z, before = [(z + n) % 4 for n in (1, 2, 3)]
    to_after, to_across, to_before = [{"grp": n} for n in (after, across_z, before)]
    far_out = send(sketch.at[across_z, top], relay.at[0], 0, 0, to_after)
    far_home = send(sketch.at[across_z, bottom], relay.at[1], 1, 1, to_before)
    near_out = send(sketch.at[after, bottom], parts.at[0], 2, 2, to_after)
    near_home = send(sketch.at[before, top], parts.at[1], 3, 3, to_before)
    joint_out = send(sketch.at[after, top], parts.at[2], 4, 4, to_after)
    joint_home = send(sketch.at[before, bottom], parts.at[3], 5, 5, to_before)

    def leaf_step(n, carry):
        sketch_leaf((z + jnp.where(n == 0, 2, jnp.where(n == 1, 1, jnp.where(n == 2, 3, 0)))) % 4)

        @pl.when(n == 0)
        def _():
            far_out.start()
            far_home.start()

        @pl.when(n == 1)
        def _():
            near_out.start()

        @pl.when(n == 2)
        def _():
            near_home.start()

        return carry

    lax.fori_loop(0, 4, leaf_step, 0)
    far_out.wait_recv()
    sketch[after, 0:128] = sketch[after, 0:128] + relay[0]
    joint_out.start()
    far_home.wait_recv()
    sketch[before, 128:256] = sketch[before, 128:256] + relay[1]
    joint_home.start()
    near_out.wait_recv()
    near_home.wait_recv()
    joint_out.wait_recv()
    whole[0:128] = sketch[z, 0:128] + parts[1] + parts[2]
    joint_home.wait_recv()
    whole[128:256] = sketch[z, 128:256] + parts[0] + parts[3]
    flat = whole[...]
    leaf_gram[z] = lax.dot_general(
        flat.T, flat, (((1,), (0,)), ((), ())), precision=precise, preferred_element_type=jnp.float32
    )
    others = ((2, across_z, to_across), (1, after, to_after), (3, before, to_before))
    gram_sends = [send(leaf_gram.at[z], leaf_gram.at[z], 5 + n, 6 + z, peer) for n, _, peer in others]
    row_sends = [
        send(whole.at[pl.ds(pl.multiple_of(there * 64, 64), 64)], leaf_rows.at[z], 8 + n, 10 + z, peer)
        for n, there, peer in others
    ]
    for copy in gram_sends:
        copy.start()
    leaf_rows[z] = whole[pl.ds(pl.multiple_of(z * 64, 64), 64)]
    for _, there, peer in others:
        send(leaf_gram.at[there], leaf_gram.at[there], 6, 6 + there, peer).wait_recv()
    first_pair = leaf_gram[0] + leaf_gram[1]
    second_pair = leaf_gram[2] + leaf_gram[3]
    own_top = first_pair + second_pair
    top_gram[...] = own_top

    def tree_send(slot, target):
        return send(top_gram, tree.at[e], 12 + slot, 14 + e, {"dev": me // 8 * 8 + target})

    tree_sends = (
        (e != 7, tree_send(0, 7)),
        (e != 3, tree_send(1, 3)),
        (e % 4 != 1, tree_send(2, e // 4 * 4 + 1)),
        (e % 2 == 1, tree_send(3, e - 1)),
    )
    for needed, copy in tree_sends:
        pl.when(needed)(copy.start)
    for copy in row_sends:
        copy.start()
    for m, gram in enumerate([leaf_gram[c] for c in range(4)] + [first_pair, second_pair, own_top]):
        init_work(work, m, gram)
    factor_span(work, range(7), SEGS[:2])

    def arrived(slot):
        send(top_gram, tree.at[slot], 12, 14 + slot, to_after).wait_recv()
        return tree[slot]

    def keep(left, right):
        children[0] = left
        children[1] = right

    def eight_send(slot, row):
        return send(top_gram, eights.at[y_at], 16 + slot, 22 + y_at, {"dev": row * 8 + 7})

    eight_sends = (
        (e * 4 + y_at == 28, eight_send(0, 1)),
        (e * 4 + y_at == 29, eight_send(0, 0)),
        (e * 4 + y_at == 30, eight_send(0, 1)),
        (e * 4 + y_at == 31, eight_send(0, 1)),
        (e * 4 + y_at == 31, eight_send(1, 2)),
    )

    @pl.when(e == 7)
    def _():
        pairs = [arrived(0) + arrived(1), arrived(2) + arrived(3), arrived(4) + arrived(5), arrived(6) + own_top]
        for needed, copy in tree_sends:
            pl.when(needed)(copy.wait_send)
        eight = (pairs[0] + pairs[1]) + (pairs[2] + pairs[3])
        top_gram[...] = eight
        for needed, copy in eight_sends:
            pl.when(needed)(copy.start)

    factor_span(work, range(7), SEGS[2:])
    for _, there, peer in others:
        send(leaf_rows.at[there], leaf_rows.at[there], 9, 10 + there, peer).wait_recv()
    results = [
        pltpu.make_async_copy(work.at[pl.ds(0, 7)], state_ref, load_sem.at[0]),
        pltpu.make_async_copy(leaf_rows, rows_ref, load_sem.at[1]),
        pltpu.make_async_copy(children, child_ref, load_sem.at[2]),
    ]
    results[0].start()
    results[1].start()

    @pl.when(e % 2 == 0)
    def _():
        keep(own_top, arrived(e + 1))

    @pl.when(e % 4 == 1)
    def _():
        keep(arrived(e - 1) + own_top, arrived(e + 1) + arrived(e + 2))

    @pl.when(e == 3)
    def _():
        left = arrived(0) + arrived(1) + (arrived(2) + own_top)
        keep(left, arrived(4) + arrived(5) + (arrived(6) + arrived(7)))

    @pl.when(e == 7)
    def _():
        eight = top_gram[...]

        def landed(row):
            send(top_gram, eights.at[row], 16, 22 + row, to_after).wait_recv()
            return eights[row]

        @pl.when(y_at == 0)
        def _():
            keep(eight, landed(1))

        @pl.when(y_at == 1)
        def _():
            keep(landed(0) + eight, landed(2) + landed(3))

        @pl.when(y_at == 2)
        def _():
            keep(eight, landed(3))

        @pl.when(y_at == 3)
        def _():
            keep(eight, eight)

        for needed, copy in eight_sends:
            pl.when(needed)(copy.wait_send)

    @pl.when(e != 7)
    def _():
        for needed, copy in tree_sends:
            pl.when(needed)(copy.wait_send)

    results[2].start()
    for copy in [far_out, far_home, near_out, near_home, joint_out, joint_home] + gram_sends + row_sends:
        copy.wait_send()
    for way in range(4):
        span = pl.ds(0, 15)
        pltpu.make_async_remote_copy(
            src_ref=probe.at[span], dst_ref=probe.at[span], send_sem=send_sem.at[way], recv_sem=recv_sem.at[0],
            device_id={"dev": targets[way]}, device_id_type=pl.DeviceIdType.MESH,
        ).wait_send()
    span = pl.ds(0, 64)
    pltpu.make_async_remote_copy(
        src_ref=probe.at[span], dst_ref=probe.at[span], send_sem=send_sem.at[ACROSS], recv_sem=recv_sem.at[0],
        device_id={"dev": partner}, device_id_type=pl.DeviceIdType.MESH,
    ).wait_send()
    for result in results:
        result.wait()


def sum_and_factor(columns, ranks, omega, u_rows, v_rows):
    smem = pl.BlockSpec(memory_space=pltpu.SMEM)
    anywhere = pl.BlockSpec(memory_space=pl.ANY)
    return pl.pallas_call(
        sum_kernel,
        out_shape=(
            jax.ShapeDtypeStruct((7, 128, 256), jnp.float32),
            jax.ShapeDtypeStruct((4, 64, 128), jnp.float32),
            jax.ShapeDtypeStruct((2, 128, 128), jnp.float32),
        ),
        in_specs=[pl.BlockSpec(memory_space=pltpu.VMEM), smem, anywhere, anywhere, anywhere],
        out_specs=(anywhere, anywhere, anywhere),
        scratch_shapes=[
            pltpu.VMEM((128, 256, 128), jnp.float32),
            pltpu.VMEM((320, 32, 256), jnp.float32),
            pltpu.VMEM((320, 32, 256), jnp.float32),
            pltpu.VMEM((4, 256, 2560), jnp.bfloat16),
            pltpu.VMEM((4, 256, 2560), jnp.bfloat16),
            pltpu.VMEM((384, 32, 256), jnp.bfloat16),
            pltpu.VMEM((2560, 256), jnp.bfloat16),
            pltpu.VMEM((4, 256, 128), jnp.float32),
            pltpu.VMEM((2, 128, 128), jnp.float32),
            pltpu.VMEM((4, 128, 128), jnp.float32),
            pltpu.VMEM((256, 128), jnp.float32),
            pltpu.VMEM((4, 128, 128), jnp.float32),
            pltpu.VMEM((4, 64, 128), jnp.float32),
            pltpu.VMEM((128, 128), jnp.float32),
            pltpu.VMEM((8, 128, 128), jnp.float32),
            pltpu.VMEM((4, 128, 128), jnp.float32),
            pltpu.VMEM((7, 128, 256), jnp.float32),
            pltpu.VMEM((2, 128, 128), jnp.float32),
            pltpu.VMEM((8, 128), jnp.int32),
            pltpu.VMEM((8, 128), jnp.int32),
            pltpu.VMEM((8, 128), jnp.int32),
            pltpu.SMEM((8, 128), jnp.int32),
            pltpu.SMEM((8, 128), jnp.int32),
            pltpu.SemaphoreType.DMA((5,)),
            pltpu.SemaphoreType.DMA((5,)),
            pltpu.SemaphoreType.DMA((128,)),
            pltpu.SemaphoreType.DMA((18,)),
            pltpu.SemaphoreType.DMA((26,)),
        ],
        compiler_params=pltpu.CompilerParams(
            collective_id=0, has_side_effects=True, vmem_limit_bytes=62 * 2**20
        ),
        name="recompress",
    )(columns, ranks, omega, u_rows, v_rows)


def finish_kernel(child_ref, state_ref, rows_ref, basis_ref, transfer_ref, work, rows, basis, transfer, sem):
    loads = [
        pltpu.make_async_copy(state_ref, work.at[pl.ds(0, 7)], sem.at[0]),
        pltpu.make_async_copy(rows_ref, rows, sem.at[1]),
    ]
    for load in loads:
        load.start()
    init_work(work, 7, child_ref[0])
    init_work(work, 8, child_ref[1])
    init_work(work, 9, child_ref[0] + child_ref[1])
    panel = make_panel(work, range(7, 10), 3)
    panel(0, 16)
    panel(1, 32)
    for load in loads:
        load.wait()
    panel(2, 48)
    for c in range(4):
        basis[c] = times_transposed(rows[c], work[c, :, 128:256])
    panel(3, 64)
    write_node(work, 0, transfer)
    panel(4, 80)
    write_node(work, 1, transfer)
    panel(5, 96)
    write_node(work, 2, transfer)
    early, late = pl.ds(0, 3), pl.ds(3, 1)
    stores = [
        pltpu.make_async_copy(basis, basis_ref, sem.at[2]),
        pltpu.make_async_copy(transfer.at[early], transfer_ref.at[early], sem.at[3]),
        pltpu.make_async_copy(transfer.at[late], transfer_ref.at[late], sem.at[4]),
    ]
    stores[0].start()
    stores[1].start()
    panel(6, 112)
    panel(7, 128)
    write_node(work, 3, transfer)
    stores[2].start()
    for store in stores:
        store.wait()


def finish(state, rows, children):
    vmem = pl.BlockSpec(memory_space=pltpu.VMEM)
    anywhere = pl.BlockSpec(memory_space=pl.ANY)
    return pl.pallas_call(
        finish_kernel,
        out_shape=(
            jax.ShapeDtypeStruct((4, 64, 128), jnp.float32),
            jax.ShapeDtypeStruct((4, 256, 128), jnp.float32),
        ),
        in_specs=[vmem, anywhere, anywhere],
        out_specs=(anywhere, anywhere),
        scratch_shapes=[
            pltpu.VMEM((10, 128, 256), jnp.float32),
            pltpu.VMEM((4, 64, 128), jnp.float32),
            pltpu.VMEM((4, 64, 128), jnp.float32),
            pltpu.VMEM((4, 256, 128), jnp.float32),
            pltpu.SemaphoreType.DMA((5,)),
        ],
        compiler_params=pltpu.CompilerParams(vmem_limit_bytes=62 * 2**20),
        name="finish",
    )(children, state, rows)


def on_device(omega, u_factor, v_factor, columns, ranks):
    u_rows = jnp.swapaxes(u_factor, 3, 4).reshape(320, 32, 256)
    v_rows = jnp.swapaxes(v_factor, 3, 4).reshape(320, 32, 256)
    named = jnp.swapaxes(columns[0], 1, 2)
    state, rows, children = sum_and_factor(named, ranks[0], omega[0], u_rows, v_rows)
    return finish(state, rows, children)


def solution(mesh):
    placed = (
        P("grp", "dev", None, None),
        P("grp", "dev", None, None, None),
        P("grp", "dev", None, None, None),
        P("grp", "dev", None, None),
        P("grp", "dev", None),
    )
    return jax.shard_map(
        on_device,
        mesh=mesh,
        in_specs=placed,
        out_specs=(P("dev", "grp", None), P("dev", None, None)),
        check_vma=False,
    )
```

```python
import functools
import jax
import jax.numpy as jnp
from jax import lax
from jax.experimental import pallas as pl
from jax.experimental.pallas import tpu as pltpu
from jax.sharding import PartitionSpec as P

precise = lax.Precision.HIGHEST


def pick_lane(x, lane):
    idx = jnp.full(x.shape, lane, jnp.int32)
    return jnp.take_along_axis(x, idx, axis=1)


def make_panel(work, mats, group):
    sub = lax.broadcasted_iota(jnp.int32, (8, 128), 0)
    lane = lax.broadcasted_iota(jnp.int32, (8, 128), 1)

    def split(x):
        h = x.astype(jnp.bfloat16).astype(jnp.float32)
        rest = x - h
        d = rest.astype(jnp.bfloat16).astype(jnp.float32)
        return h, d, rest - d

    def panel(k, top):
        base = k * 16 if isinstance(k, int) else pl.multiple_of(k * 16, 16)
        raw = [work[m, pl.ds(base, 16), :] for m in mats]
        prods = []
        rows = []
        for g in range(0, len(mats), group):
            part = raw[g : g + group]
            ps = [[x[0:8, 0:128], x[8:16, 0:128]] for x in part]
            qs = [[x[0:8, 128:256], x[8:16, 128:256]] for x in part]
            high = [[pick_lane(p[0], base + r) for r in range(8)] for p in ps]
            low = [[pick_lane(p[1], base + r) for r in range(16)] for p in ps]
            for r in range(16):
                h, n = r // 8, r % 8
                for p, q, up, down in zip(ps, qs, high, low):
                    pivot = (up if h == 0 else down)[r][n : n + 1]
                    inv = lax.rsqrt(jnp.broadcast_to(pivot, (8, 128)))
                    prow = p[h][n : n + 1] * inv
                    qrow = q[h][n : n + 1] * inv
                    below = down[r] * inv
                    if h == 0:
                        here = up[r] * inv
                        p[1] = p[1] - below * prow
                        q[1] = q[1] - below * qrow
                        for t in range(r + 1, 8):
                            up[t] = up[t] - here * here[t : t + 1]
                            down[t] = down[t] - below * here[t : t + 1]
                    else:
                        here = below
                    for t in range(max(r + 1, 8), 16):
                        down[t] = down[t] - below * below[t - 8 : t - 7]
                    rest = jnp.where(sub > n, here, 0.0)
                    p[h] = jnp.where(sub == n, prow, p[h] - rest * prow)
                    q[h] = jnp.where(sub == n, qrow, q[h] - rest * qrow)
            for p, q in zip(ps, qs):
                both = [jnp.where(lane >= base + 8 * h + sub, p[h], 0.0) for h in range(2)]
                full = jnp.concatenate([jnp.concatenate(both, axis=0), jnp.concatenate(q, axis=0)], axis=1)
                rows.append(full)
                if top == 128:
                    continue
                after = [jnp.where(lane >= base + 16, x, 0.0) for x in both]
                ph, pd, pe = split(jnp.concatenate(after, axis=0))
                fh, fd, fe = split(full)
                left = jnp.concatenate([ph, ph, pd, ph, pe, pd], axis=0)
                right = jnp.concatenate([fh, fd, fh, fe, fh, fd], axis=0)
                turned = left.T[top:].astype(jnp.bfloat16)
                prods.append(
                    lax.dot_general(
                        turned,
                        right.astype(jnp.bfloat16),
                        (((1,), (0,)), ((), ())),
                        preferred_element_type=jnp.float32,
                    )
                )
        for m, full in zip(mats, rows):
            work[m, pl.ds(base, 16), :] = full
        for m, prod in zip(mats, prods):
            work[m, top:128, :] = work[m, top:128, :] - prod

    return panel


def init_work(work, m, gram):
    r = lax.broadcasted_iota(jnp.int32, (128, 128), 0)
    c = lax.broadcasted_iota(jnp.int32, (128, 128), 1)
    work[m, :, 0:128] = gram
    work[m, :, 128:256] = jnp.where(r == c, 1.0, 0.0)


NODES = ((0, 1, 4), (2, 3, 5), (4, 5, 6), (7, 8, 9))


def times_transposed(x, y):
    return lax.dot_general(x, y, (((1,), (1,)), ((), ())), precision=precise, preferred_element_type=jnp.float32)


def write_node(work, n, transfer_ref):
    left, right, parent = NODES[n]
    inverse = work[parent, :, 128:256]
    for half, child in enumerate((left, right)):
        made = times_transposed(work[child, :, 0:128], inverse)
        if n == 3:
            made = jnp.where(lax.axis_index("dev") == lax.axis_size("dev") - 1, 0.0, made)
        transfer_ref[n, half * 128 : (half + 1) * 128, :] = made


RIGHT, LEFT, DOWN, UP, ACROSS = range(5)


def split_two(x):
    high = x.astype(jnp.bfloat16)
    low = (x - high.astype(jnp.float32)).astype(jnp.bfloat16)
    return high, low


def bf16_dot(x, y):
    return lax.dot_general(x, y, (((1,), (0,)), ((), ())), preferred_element_type=jnp.float32)


def sort_blocks(column_ref, named, places, slots):
    lane = lax.broadcasted_iota(jnp.int32, (128, 128), 1)
    down = lax.broadcasted_iota(jnp.int32, (128, 128), 0)
    named[...] = jnp.full((8, 128), -1, jnp.int32)
    for i in range(4):
        named[i : i + 1, 0:80] = column_ref[i]
    rows = named[...]
    turned = rows.T
    places[...] = jnp.full((8, 128), -1, jnp.int32)
    for i in range(4):
        row = jnp.broadcast_to(rows[i : i + 1], (128, 128))
        turn = ((turned[:, i : i + 1] == row) & (down < lane)).astype(jnp.int32)
        for other in range(i):
            turn = turn + (turned[:, other : other + 1] == row).astype(jnp.int32)
        place = jnp.minimum(jnp.sum(turn, axis=0, keepdims=True), 2) * 128 + rows[i : i + 1]
        places[i : i + 1] = jnp.where(lane[0:1] < 80, place, -1)
    turned = places[...].T
    slots[...] = jnp.zeros((8, 128), jnp.int32)
    for t in range(3):
        block = jnp.zeros((128, 128), jnp.int32)
        for i in range(4):
            block = block + jnp.where(turned[:, i : i + 1] == lane + t * 128, down + i * 80, 0)
        slots[t : t + 1] = jnp.minimum(jnp.sum(block, axis=0, keepdims=True), 319)


def sum_kernel(
    column_ref, rank_ref, omega_ref, u_ref, v_ref, state_ref, rows_ref, child_ref,
    probe, u_all, v_all, u_high, u_low, coeff, weights,
    sketch, relay, parts, whole, leaf_gram, leaf_rows, top_gram, tree, eights, work, children,
    named, places, slots, place_at, slot_at,
    load_sem, send_sem, recv_sem, out_sem, in_sem,
):
    me = lax.axis_index("dev")
    core = me % 2
    x_at = me // 2 % 4
    y_at = me // 8
    partner = me + 1 - 2 * core

    def device(dy, dx):
        return ((y_at + dy) % 4 * 4 + (x_at + dx) % 4) * 2 + core

    targets = (device(0, 1), device(0, 3), device(1, 0), device(3, 0), partner)
    own = pltpu.make_async_copy(omega_ref, probe.at[pl.ds(me * 4, 4)], load_sem.at[0])
    own.start()
    loads = [
        pltpu.make_async_copy(v_ref, v_all, load_sem.at[1]),
        pltpu.make_async_copy(u_ref, u_all, load_sem.at[2]),
    ]
    for load in loads:
        load.start()
    z = lax.axis_index("grp")
    e = me % 8
    barrier = pltpu.get_barrier_semaphore()
    peers = [{"dev": me // 8 * 8 + (e + n) % 8} for n in range(1, 8)]
    peers += [{"dev": (me + 8 * n) % 32} for n in range(1, 4)]
    peers += [{"grp": (z + n) % 4} for n in range(1, 4)]
    for peer in peers:
        pl.semaphore_signal(barrier, inc=1, device_id=peer, device_id_type=pl.DeviceIdType.MESH)
    sort_blocks(column_ref, named, places, slots)
    tables = [
        pltpu.make_async_copy(places, place_at, load_sem.at[3]),
        pltpu.make_async_copy(slots, slot_at, load_sem.at[4]),
    ]
    pl.semaphore_wait(barrier, 13)
    own.wait()
    for table in tables:
        table.start()

    def move(cluster, way):
        return pltpu.make_async_remote_copy(
            src_ref=probe.at[cluster],
            dst_ref=probe.at[cluster],
            send_sem=send_sem.at[way],
            recv_sem=recv_sem.at[cluster],
            device_id={"dev": targets[way]},
            device_id_type=pl.DeviceIdType.MESH,
        )

    def await_cluster(cluster):
        move(cluster, RIGHT).wait_recv()

    def make_coeff(cluster):
        wide = jnp.concatenate(split_two(probe[cluster]), axis=1)
        rows = jnp.concatenate([v_all[slot_at[t, cluster]] for t in range(3)], axis=0)
        high, low = split_two(rows)
        both = bf16_dot(high, wide)
        made = both[:, 0:128] + both[:, 128:256] + bf16_dot(low, wide[:, 0:128])
        packed = jnp.concatenate(split_two(made), axis=1)
        for t in range(3):
            coeff[t * 128 + cluster] = packed[t * 32 : t * 32 + 32]

    rank_row = lax.broadcasted_iota(jnp.int32, (32, 256), 0)

    def turn_rows(chunk):
        pieces = [
            jnp.where(rank_row < rank_ref[chunk // 10, chunk % 10 * 8 + e], u_all[chunk * 8 + e], 0.0) for e in range(8)
        ]
        high, low = split_two(jnp.concatenate(pieces, axis=0).T)
        leaf = chunk // 10
        where = pl.ds(pl.multiple_of(chunk % 10 * 256, 256), 256)
        u_high[leaf, :, where] = high
        u_low[leaf, :, where] = low

    def step(dy, dx, j, before, first=False, chunk=None):
        along_x = device(dy, dx) * 4 + j
        along_y = device(dx, dy) * 4 + j + 2
        flips = ((along_x, (RIGHT, LEFT, DOWN, UP)), (along_y, (DOWN, UP, RIGHT, LEFT)))
        for cluster, (ahead, back, out, home) in flips:
            if not first:
                await_cluster(cluster)
            ways = []
            if isinstance(dy, int) and dy == 0:
                if first:
                    ways += [ahead, back]
                elif dx == 3 and j == 0:
                    ways += [ahead]
                elif dx == 1 and j == 1:
                    ways += [back]
                ways += [out, home]
            elif dy == 3 and j == 0:
                ways += [out]
            elif dy == 1 and j == 1:
                ways += [home]
            for way in ways + [ACROSS]:
                move(cluster, way).start()
        now = [along_x, along_y]
        work = list(now)
        if before is not None:
            for cluster in before:
                await_cluster(cluster)
                work.append(cluster)
        if first and j == 0:
            loads[0].wait()
            for table in tables:
                table.wait()
        for cluster in work:
            make_coeff(cluster)
        if chunk is not None:
            turn_rows(chunk)
            turn_rows(chunk + 1)
        shift = 4 - 8 * core
        return [c + shift for c in now]

    late = step(0, 0, 0, None, first=True)
    late = step(0, 0, 1, late, first=True)
    loads[1].wait()

    def turn_some(chunk, carry):
        turn_rows(chunk)
        return carry

    lax.fori_loop(0, 8, turn_some, 0)
    for dx, j in ((3, 0), (1, 1), (3, 1), (1, 0), (2, 0), (2, 1)):
        late = step(0, dx, j, late)

    def far(q):
        return jnp.where(q == 0, 0, jnp.where(q == 1, 3, q - 1))

    def cross(q, late):
        for s, (dy, j) in enumerate(((3, 0), (1, 1), (3, 1), (1, 0))):
            late = step(dy, far(q), j, late, chunk=8 + q * 8 + s * 2)
        return tuple(late)

    def end(q, late):
        for j in range(2):
            late = step(2, far(q), j, late)
        return tuple(late)

    late = lax.fori_loop(0, 4, cross, tuple(late))
    late = lax.fori_loop(0, 4, end, late)
    for cluster in late:
        await_cluster(cluster)
    for cluster in late:
        make_coeff(cluster)

    def sketch_leaf(leaf):
        for b in range(80):
            weights[b * 32 : b * 32 + 32, :] = coeff[place_at[leaf, b]]
        both = bf16_dot(u_high[leaf], weights[...])
        sketch[leaf] = both[:, 0:128] + both[:, 128:256] + bf16_dot(u_low[leaf], weights[:, 0:128])

    def send(source, target, out, arrival, peer):
        return pltpu.make_async_remote_copy(
            src_ref=source,
            dst_ref=target,
            send_sem=out_sem.at[out],
            recv_sem=in_sem.at[arrival],
            device_id=peer,
            device_id_type=pl.DeviceIdType.MESH,
        )

    top, bottom = pl.ds(0, 128), pl.ds(128, 128)
    after, across_z, before = [(z + n) % 4 for n in (1, 2, 3)]
    to_after, to_across, to_before = [{"grp": n} for n in (after, across_z, before)]
    halves = [(pl.ds(64 * h, 64), pl.ds(128 + 64 * h, 64), h) for h in range(2)]
    far_out = [send(sketch.at[across_z, a], relay.at[0, a], 18 * h, 26 * h, to_after) for a, _, h in halves]
    far_home = [
        send(sketch.at[across_z, b], relay.at[1, a], 1 + 18 * h, 1 + 26 * h, to_before) for a, b, h in halves
    ]
    near_out = send(sketch.at[after, bottom], parts.at[0], 2, 2, to_after)
    near_home = send(sketch.at[before, top], parts.at[1], 3, 3, to_before)
    joint_out = [send(sketch.at[after, a], parts.at[2, a], 4 + 16 * h, 4 + 24 * h, to_after) for a, _, h in halves]
    joint_home = [
        send(sketch.at[before, b], parts.at[3, a], 5 + 16 * h, 5 + 24 * h, to_before) for a, b, h in halves
    ]

    def leaf_step(n, carry):
        sketch_leaf((z + jnp.where(n == 0, 2, jnp.where(n == 1, 1, jnp.where(n == 2, 3, 0)))) % 4)

        @pl.when(n == 0)
        def _():
            for copy in (far_out[0], far_home[0], far_out[1], far_home[1]):
                copy.start()

        @pl.when(n == 1)
        def _():
            near_out.start()

        @pl.when(n == 2)
        def _():
            near_home.start()

        return carry

    lax.fori_loop(0, 4, leaf_step, 0)
    for h in range(2):
        lo, hi = 64 * h, 64 * h + 64
        far_out[h].wait_recv()
        sketch[after, lo:hi] = sketch[after, lo:hi] + relay[0, lo:hi]
        joint_out[h].start()
        far_home[h].wait_recv()
        sketch[before, 128 + lo : 128 + hi] = sketch[before, 128 + lo : 128 + hi] + relay[1, lo:hi]
        joint_home[h].start()
    near_out.wait_recv()
    near_home.wait_recv()
    for copy in joint_out:
        copy.wait_recv()
    whole[0:128] = sketch[z, 0:128] + parts[1] + parts[2]
    for copy in joint_home:
        copy.wait_recv()
    whole[128:256] = sketch[z, 128:256] + parts[0] + parts[3]
    flat = whole[...]
    leaf_gram[z] = lax.dot_general(
        flat.T, flat, (((1,), (0,)), ((), ())), precision=precise, preferred_element_type=jnp.float32
    )
    others = ((2, across_z, to_across), (1, after, to_after), (3, before, to_before))
    gram_sends = [send(leaf_gram.at[z], leaf_gram.at[z], 5 + n, 6 + z, peer) for n, _, peer in others]
    row_sends = [
        send(whole.at[pl.ds(pl.multiple_of(there * 64, 64), 64)], leaf_rows.at[z], 8 + n, 10 + z, peer)
        for n, there, peer in others
    ]
    for copy in gram_sends:
        copy.start()
    leaf_rows[z] = whole[pl.ds(pl.multiple_of(z * 64, 64), 64)]
    for _, there, peer in others:
        send(leaf_gram.at[there], leaf_gram.at[there], 6, 6 + there, peer).wait_recv()
    first_pair = leaf_gram[0] + leaf_gram[1]
    second_pair = leaf_gram[2] + leaf_gram[3]
    own_top = first_pair + second_pair
    top_gram[...] = own_top

    def tree_send(slot, target):
        return send(top_gram, tree.at[e], 12 + slot, 14 + e, {"dev": me // 8 * 8 + target})

    tree_sends = (
        (e != 7, tree_send(0, 7)),
        (e != 3, tree_send(1, 3)),
        (e % 4 != 1, tree_send(2, e // 4 * 4 + 1)),
        (e % 2 == 1, tree_send(3, e - 1)),
    )
    for needed, copy in tree_sends:
        pl.when(needed)(copy.start)
    for copy in row_sends:
        copy.start()
    for m, gram in enumerate([leaf_gram[c] for c in range(4)] + [first_pair, second_pair, own_top]):
        init_work(work, m, gram)
    panel = make_panel(work, range(7), 7)
    for k in range(4):
        panel(k, k * 16 + 16)

    def arrived(slot):
        send(top_gram, tree.at[slot], 12, 14 + slot, to_after).wait_recv()
        return tree[slot]

    def keep(left, right):
        children[0] = left
        children[1] = right

    def eight_send(slot, row):
        return send(top_gram, eights.at[y_at], 16 + slot, 22 + y_at, {"dev": row * 8 + 7})

    eight_sends = (
        (e * 4 + y_at == 28, eight_send(0, 1)),
        (e * 4 + y_at == 29, eight_send(0, 0)),
        (e * 4 + y_at == 30, eight_send(0, 1)),
        (e * 4 + y_at == 31, eight_send(0, 1)),
        (e * 4 + y_at == 31, eight_send(1, 2)),
    )

    @pl.when(e == 7)
    def _():
        pairs = [arrived(0) + arrived(1), arrived(2) + arrived(3), arrived(4) + arrived(5), arrived(6) + own_top]
        for needed, copy in tree_sends:
            pl.when(needed)(copy.wait_send)
        eight = (pairs[0] + pairs[1]) + (pairs[2] + pairs[3])
        top_gram[...] = eight
        for needed, copy in eight_sends:
            pl.when(needed)(copy.start)

    for k in range(4, 8):
        panel(k, k * 16 + 16)
    for _, there, peer in others:
        send(leaf_rows.at[there], leaf_rows.at[there], 9, 10 + there, peer).wait_recv()
    results = [
        pltpu.make_async_copy(work.at[pl.ds(0, 7)], state_ref, load_sem.at[0]),
        pltpu.make_async_copy(leaf_rows, rows_ref, load_sem.at[1]),
        pltpu.make_async_copy(children, child_ref, load_sem.at[2]),
    ]
    results[0].start()
    results[1].start()

    @pl.when(e % 2 == 0)
    def _():
        keep(own_top, arrived(e + 1))

    @pl.when(e % 4 == 1)
    def _():
        keep(arrived(e - 1) + own_top, arrived(e + 1) + arrived(e + 2))

    @pl.when(e == 3)
    def _():
        left = arrived(0) + arrived(1) + (arrived(2) + own_top)
        keep(left, arrived(4) + arrived(5) + (arrived(6) + arrived(7)))

    @pl.when(e == 7)
    def _():
        eight = top_gram[...]

        def landed(row):
            send(top_gram, eights.at[row], 16, 22 + row, to_after).wait_recv()
            return eights[row]

        @pl.when(y_at == 0)
        def _():
            keep(eight, landed(1))

        @pl.when(y_at == 1)
        def _():
            keep(landed(0) + eight, landed(2) + landed(3))

        @pl.when(y_at == 2)
        def _():
            keep(eight, landed(3))

        @pl.when(y_at == 3)
        def _():
            keep(eight, eight)

        for needed, copy in eight_sends:
            pl.when(needed)(copy.wait_send)

    @pl.when(e != 7)
    def _():
        for needed, copy in tree_sends:
            pl.when(needed)(copy.wait_send)

    results[2].start()
    for copy in far_out + far_home + [near_out, near_home] + joint_out + joint_home + gram_sends + row_sends:
        copy.wait_send()
    for way in range(4):
        span = pl.ds(0, 15)
        pltpu.make_async_remote_copy(
            src_ref=probe.at[span], dst_ref=probe.at[span], send_sem=send_sem.at[way], recv_sem=recv_sem.at[0],
            device_id={"dev": targets[way]}, device_id_type=pl.DeviceIdType.MESH,
        ).wait_send()
    span = pl.ds(0, 64)
    pltpu.make_async_remote_copy(
        src_ref=probe.at[span], dst_ref=probe.at[span], send_sem=send_sem.at[ACROSS], recv_sem=recv_sem.at[0],
        device_id={"dev": partner}, device_id_type=pl.DeviceIdType.MESH,
    ).wait_send()
    for result in results:
        result.wait()


def sum_and_factor(columns, ranks, omega, u_rows, v_rows):
    smem = pl.BlockSpec(memory_space=pltpu.SMEM)
    anywhere = pl.BlockSpec(memory_space=pl.ANY)
    return pl.pallas_call(
        sum_kernel,
        out_shape=(
            jax.ShapeDtypeStruct((7, 128, 256), jnp.float32),
            jax.ShapeDtypeStruct((4, 64, 128), jnp.float32),
            jax.ShapeDtypeStruct((2, 128, 128), jnp.float32),
        ),
        in_specs=[pl.BlockSpec(memory_space=pltpu.VMEM), smem, anywhere, anywhere, anywhere],
        out_specs=(anywhere, anywhere, anywhere),
        scratch_shapes=[
            pltpu.VMEM((128, 256, 128), jnp.float32),
            pltpu.VMEM((320, 32, 256), jnp.float32),
            pltpu.VMEM((320, 32, 256), jnp.float32),
            pltpu.VMEM((4, 256, 2560), jnp.bfloat16),
            pltpu.VMEM((4, 256, 2560), jnp.bfloat16),
            pltpu.VMEM((384, 32, 256), jnp.bfloat16),
            pltpu.VMEM((2560, 256), jnp.bfloat16),
            pltpu.VMEM((4, 256, 128), jnp.float32),
            pltpu.VMEM((2, 128, 128), jnp.float32),
            pltpu.VMEM((4, 128, 128), jnp.float32),
            pltpu.VMEM((256, 128), jnp.float32),
            pltpu.VMEM((4, 128, 128), jnp.float32),
            pltpu.VMEM((4, 64, 128), jnp.float32),
            pltpu.VMEM((128, 128), jnp.float32),
            pltpu.VMEM((8, 128, 128), jnp.float32),
            pltpu.VMEM((4, 128, 128), jnp.float32),
            pltpu.VMEM((7, 128, 256), jnp.float32),
            pltpu.VMEM((2, 128, 128), jnp.float32),
            pltpu.VMEM((8, 128), jnp.int32),
            pltpu.VMEM((8, 128), jnp.int32),
            pltpu.VMEM((8, 128), jnp.int32),
            pltpu.SMEM((8, 128), jnp.int32),
            pltpu.SMEM((8, 128), jnp.int32),
            pltpu.SemaphoreType.DMA((5,)),
            pltpu.SemaphoreType.DMA((5,)),
            pltpu.SemaphoreType.DMA((128,)),
            pltpu.SemaphoreType.DMA((22,)),
            pltpu.SemaphoreType.DMA((30,)),
        ],
        compiler_params=pltpu.CompilerParams(
            collective_id=0, has_side_effects=True, vmem_limit_bytes=62 * 2**20
        ),
        name="recompress",
    )(columns, ranks, omega, u_rows, v_rows)


def finish_kernel(child_ref, state_ref, rows_ref, basis_ref, transfer_ref, work, rows, basis, transfer, sem):
    loads = [
        pltpu.make_async_copy(state_ref, work.at[pl.ds(0, 7)], sem.at[0]),
        pltpu.make_async_copy(rows_ref, rows, sem.at[1]),
    ]
    for load in loads:
        load.start()
    init_work(work, 7, child_ref[0])
    init_work(work, 8, child_ref[1])
    init_work(work, 9, child_ref[0] + child_ref[1])
    panel = make_panel(work, range(7, 10), 3)
    panel(0, 16)
    panel(1, 32)
    for load in loads:
        load.wait()
    panel(2, 48)
    for c in range(4):
        basis[c] = times_transposed(rows[c], work[c, :, 128:256])
    panel(3, 64)
    write_node(work, 0, transfer)
    panel(4, 80)
    write_node(work, 1, transfer)
    panel(5, 96)
    write_node(work, 2, transfer)
    early, late = pl.ds(0, 3), pl.ds(3, 1)
    stores = [
        pltpu.make_async_copy(basis, basis_ref, sem.at[2]),
        pltpu.make_async_copy(transfer.at[early], transfer_ref.at[early], sem.at[3]),
        pltpu.make_async_copy(transfer.at[late], transfer_ref.at[late], sem.at[4]),
    ]
    stores[0].start()
    stores[1].start()
    panel(6, 112)
    panel(7, 128)
    write_node(work, 3, transfer)
    stores[2].start()
    for store in stores:
        store.wait()


def finish(state, rows, children):
    vmem = pl.BlockSpec(memory_space=pltpu.VMEM)
    anywhere = pl.BlockSpec(memory_space=pl.ANY)
    return pl.pallas_call(
        finish_kernel,
        out_shape=(
            jax.ShapeDtypeStruct((4, 64, 128), jnp.float32),
            jax.ShapeDtypeStruct((4, 256, 128), jnp.float32),
        ),
        in_specs=[vmem, anywhere, anywhere],
        out_specs=(anywhere, anywhere),
        scratch_shapes=[
            pltpu.VMEM((10, 128, 256), jnp.float32),
            pltpu.VMEM((4, 64, 128), jnp.float32),
            pltpu.VMEM((4, 64, 128), jnp.float32),
            pltpu.VMEM((4, 256, 128), jnp.float32),
            pltpu.SemaphoreType.DMA((5,)),
        ],
        compiler_params=pltpu.CompilerParams(vmem_limit_bytes=62 * 2**20),
        name="finish",
    )(children, state, rows)


def on_device(omega, u_factor, v_factor, columns, ranks):
    u_rows = jnp.swapaxes(u_factor, 3, 4).reshape(320, 32, 256)
    v_rows = jnp.swapaxes(v_factor, 3, 4).reshape(320, 32, 256)
    named = jnp.swapaxes(columns[0], 1, 2)
    state, rows, children = sum_and_factor(named, ranks[0], omega[0], u_rows, v_rows)
    return finish(state, rows, children)


def solution(mesh):
    placed = (
        P("grp", "dev", None, None),
        P("grp", "dev", None, None, None),
        P("grp", "dev", None, None, None),
        P("grp", "dev", None, None),
        P("grp", "dev", None),
    )
    return jax.shard_map(
        on_device,
        mesh=mesh,
        in_specs=placed,
        out_specs=(P("dev", "grp", None), P("dev", None, None)),
        check_vma=False,
    )
```
